128 devices in a mesh: row: 8 (over x, core), col: 16 (over y, z).
Axes of the slice: x: 4, y: 4, z: 4, core: 2. Of those that a mesh axis runs over, the one named last changes fastest.
Arguments:
- solution: float32 [49152, 128], P(('row', 'col')), may hold values from -6 to 6
- right_side: float32 [49152, 128], P(('row', 'col')), may hold values from -6 to 6
- block_values: bfloat16 [384, 64, 128, 128], P('row', 'col'), may hold values from -0.0625 to 0.0625
- block_columns: int32 [384, 64], P('row', 'col'), may hold values from 0 to 383, as said below
- row_order: int32 [49152], P(('row', 'col')), may hold values from 0 to 49151, as said below
- tri_inverses: bfloat16 [16384, 28672], P(('row', 'col')), may hold values from -1 to 2
- lower_updates: bfloat16 [12288, 16384], P(None, ('row', 'col')), may hold values from -0.0625 to 0.0625
- upper_updates: bfloat16 [16384, 12288], P(('row', 'col')), may hold values from -0.0625 to 0.0625
- update_rows: int32 [2, 16384], replicated, may hold values from 0 to 16383, as said below
Outputs:
- refined: float32 [49152, 128], P(('row', 'col'))
- residual: float32 [49152, 128], P(('row', 'col'))
The draws below stay inside these ranges and needn't reach their ends.
Inputs may be any that keep to these rules, and one draw needn't show every extreme that they name: `block_columns`: for block row i and slot s, the named block b satisfies (b // 3) % (16) == s // 4. `row_order`: each aligned block of 384 entries is a permutation of that block's own positions. `update_rows`: in row k, each aligned block of 2^k * 4096 entries holds distinct values below 2^(k+1) * 4096.
All inputs are finite; a program needn't handle non-finite values.
Results may differ from the reference program's by a relative error of at most 0.02.
Values may be sent and summed in bfloat16 or wider, within the bound.
A program may use at most 128 MiB of HBM per device.

```python
import math
import jax
import jax.numpy as jnp
from jax import lax

S = 4096
NRHS = 128
BLOCK = 128
KBC = 4
LEVELS = 3
SR = 128
ROWS_DEV = 384
NU = 49152
LEVEL_ROWS = 16384
NBR = 384
KB = 64
BPD = 3
UPD_ROWS = 12288
TRI_COLS = 28672
N_ROW = 8


def draw_block_columns(key, part):
    col_groups = KB // KBC
    row_groups = NU // (col_groups * ROWS_DEV)
    key_owner, key_within = jax.random.split(key)
    owner_row = jax.random.randint(key_owner, (NBR, KB), 0, row_groups)
    within = jax.random.randint(key_within, (NBR, KB), 0, BPD)
    col_group = lax.broadcasted_iota(jnp.int32, (NBR, KB), 1) // KBC
    return ((owner_row * col_groups + col_group) * BPD + within).astype(jnp.int32)


def draw_row_order(key, part):
    block_count = NU // ROWS_DEV
    subkeys = jax.random.split(jax.random.fold_in(key, 11), block_count)
    shuffled = jax.vmap(lambda single: jax.random.permutation(single, ROWS_DEV))(subkeys)
    offsets = (jnp.arange(block_count, dtype=jnp.int32) * ROWS_DEV)[:, None]
    return (shuffled.astype(jnp.int32) + offsets).reshape(NU)


def draw_update_rows(key, part):
    layers = []
    for depth_k in range(LEVELS - 1):
        span_rows = S * 2 ** depth_k
        fronts = LEVEL_ROWS // span_rows
        subkeys = jax.random.split(jax.random.fold_in(key, 100 + depth_k), 2 * fronts)

        def choose(key_first, key_second):
            picked = jax.random.permutation(key_first, 2 * span_rows - 1)[:span_rows - 1]
            chosen = jnp.concatenate([picked, jnp.full((1,), 2 * span_rows - 1, picked.dtype)])
            return jax.random.permutation(key_second, chosen)
        level_rows = jax.vmap(choose)(subkeys[:fronts], subkeys[fronts:])
        layers.append(level_rows.reshape(LEVEL_ROWS).astype(jnp.int32))
    return jnp.stack(layers, 0)


def draw_tri_inverses(key, part):
    key_base = jax.random.fold_in(jax.random.fold_in(key, 7), 0)
    key_diag = jax.random.fold_in(jax.random.fold_in(key, 7), 2)
    base = jnp.clip(jax.random.normal(key_base, (LEVEL_ROWS, TRI_COLS), jnp.float32), -6.0, 6.0)
    pieces = []
    for depth_k in range(LEVELS):
        span_rows = S * 2 ** depth_k
        offset_col = S * (2 ** depth_k - 1)
        segment = base[:, offset_col:offset_col + span_rows] / math.sqrt(span_rows)
        row_ids = lax.broadcasted_iota(jnp.int32, (LEVEL_ROWS, 1), 0) % span_rows
        col_ids = lax.broadcasted_iota(jnp.int32, (1, span_rows), 1)
        diagonal = jax.random.uniform(jax.random.fold_in(key_diag, depth_k), (LEVEL_ROWS, 1), jnp.float32, 1.0, 2.0)
        pieces.append(jnp.where(row_ids == col_ids, diagonal, segment))
    return jnp.concatenate(pieces, 1).astype(jnp.bfloat16)


def shard_levels(stream_key, dims, cuts, smallest, top_value):
    def one(dim, shards_of):
        heights = jax.random.uniform(jax.random.fold_in(jax.random.fold_in(stream_key, 6), dim), (shards_of,), jnp.float32, smallest / len(cuts), top_value / len(cuts))
        return jnp.repeat(jnp.exp(heights), dims[dim] // shards_of).reshape((-1,) + (1,) * (len(dims) - dim - 1))

    factor_of = one(*cuts[0])
    for cut in cuts[1:]:
        factor_of = factor_of * one(*cut)
    return factor_of


def bell_draw(key, dims, deviation, limit, cuts=(), held_as=jnp.bfloat16):
    gain = shard_levels(key, dims, cuts, -0.22, 0.18) if cuts else 1.0
    result = jax.random.normal(key, dims, jnp.float32) * deviation * gain
    return jnp.minimum(jnp.maximum(result, -limit), limit).astype(held_as)


def setup_inputs(seed: int = 0) -> dict:
    seeds = jax.random.split(jax.random.key(seed), 10)
    solution = bell_draw(seeds[0], (NU, NRHS), 1.0, 6.0, ((0, 128),), jnp.float32)
    right_side = bell_draw(seeds[1], (NU, NRHS), 1.0, 6.0, ((0, 128),), jnp.float32)
    block_values = bell_draw(seeds[2], (NBR, KB, BLOCK, BLOCK), (KB * BLOCK) ** -0.5, 0.0625, ((0, 8), (1, 16)))
    block_columns = draw_block_columns(jax.random.fold_in(seeds[9], 71), 0)
    row_order = draw_row_order(jax.random.fold_in(seeds[9], 71), 0)
    tri_inverses = draw_tri_inverses(jax.random.fold_in(seeds[9], 71), 0)
    lower_updates = bell_draw(seeds[6], (UPD_ROWS, LEVEL_ROWS), (S * N_ROW // 4) ** -0.5, 0.0625, ((1, 128),))
    upper_updates = bell_draw(seeds[7], (LEVEL_ROWS, UPD_ROWS), (S * N_ROW // 4) ** -0.5, 0.0625, ((0, 128),))
    update_rows = draw_update_rows(jax.random.fold_in(seeds[9], 71), 0)
    return dict(solution=solution, right_side=right_side, block_values=block_values, block_columns=block_columns, row_order=row_order, tri_inverses=tri_inverses, lower_updates=lower_updates, upper_updates=upper_updates, update_rows=update_rows)


def triangle_apply(tri_panel, vector, first_row, strict_lower):
    row_ids = first_row + lax.broadcasted_iota(jnp.int32, tri_panel.shape, 0)
    col_ids = lax.broadcasted_iota(jnp.int32, tri_panel.shape, 1)
    keep_mask = col_ids < row_ids if strict_lower else col_ids >= row_ids
    masked = jnp.where(keep_mask, tri_panel, jnp.zeros_like(tri_panel))
    return jnp.dot(masked, vector, preferred_element_type=jnp.float32)


def front_solve(tri_inverses, level_vector, depth_k, strict_lower):
    span_rows = S * 2 ** depth_k
    offset_col = S * (2 ** depth_k - 1)
    outputs = []
    for begin_row in range(0, LEVEL_ROWS, S):
        front_begin = (begin_row // span_rows) * span_rows
        tri_panel = tri_inverses[begin_row:begin_row + S, offset_col:offset_col + span_rows]
        vector = level_vector[front_begin:front_begin + span_rows]
        outputs.append(triangle_apply(tri_panel, vector, begin_row - front_begin, strict_lower))
    return jnp.concatenate(outputs, 0)


def parent_positions(update_rows, depth_k):
    span_rows = S * 2 ** depth_k
    places = jnp.arange(LEVEL_ROWS, dtype=jnp.int32)
    return ((places // (2 * span_rows)) * (2 * span_rows)).astype(jnp.int32) + update_rows[depth_k].astype(jnp.int32)


def reference(solution, right_side, block_values, block_columns, row_order, tri_inverses, lower_updates, upper_updates, update_rows):
    solution_blocks = solution.reshape(NBR, BLOCK, NRHS)
    applied = jnp.zeros((NBR, BLOCK, NRHS), jnp.float32)
    for slot_idx in range(KB):
        picked = solution_blocks[block_columns[:, slot_idx]]
        values = block_values[:, slot_idx].astype(jnp.float32)
        applied = applied + jnp.einsum("ikl,iln->ikn", values, picked, precision=lax.Precision.HIGHEST)
    residual = right_side - applied.reshape(NU, NRHS)
    permuted = residual[row_order]
    stacked = permuted.reshape(NU // ROWS_DEV, LEVELS, SR, NRHS)
    lowered = []
    incoming = jnp.zeros((LEVEL_ROWS, NRHS), jnp.float32)
    for depth_k in range(LEVELS):
        current = stacked[:, depth_k].reshape(LEVEL_ROWS, NRHS) - incoming
        rounded = current.astype(jnp.bfloat16)
        solved = front_solve(tri_inverses, rounded, depth_k, True) + rounded.astype(jnp.float32)
        level_lower = solved.astype(jnp.bfloat16)
        lowered.append(level_lower)
        if depth_k + 1 < LEVELS:
            span_rows = S * 2 ** depth_k
            offset_col = S * (2 ** depth_k - 1)
            partials = []
            for front_begin in range(0, LEVEL_ROWS, span_rows):
                matrix = lower_updates[offset_col:offset_col + span_rows, front_begin:front_begin + span_rows]
                partials.append(jnp.dot(matrix, level_lower[front_begin:front_begin + span_rows], preferred_element_type=jnp.float32))
            incoming = jnp.zeros((LEVEL_ROWS, NRHS), jnp.float32).at[parent_positions(update_rows, depth_k)].add(jnp.concatenate(partials, 0))
    corrections = [None] * LEVELS
    parent_values = None
    for depth_k in reversed(range(LEVELS)):
        reduced = lowered[depth_k].astype(jnp.float32)
        if depth_k + 1 < LEVELS:
            span_rows = S * 2 ** depth_k
            offset_col = S * (2 ** depth_k - 1)
            picked_rows = parent_values[parent_positions(update_rows, depth_k)]
            update_terms = []
            for front_begin in range(0, LEVEL_ROWS, span_rows):
                matrix = upper_updates[front_begin:front_begin + span_rows, offset_col:offset_col + span_rows]
                update_terms.append(jnp.dot(matrix, picked_rows[front_begin:front_begin + span_rows], preferred_element_type=jnp.float32))
            reduced = reduced - jnp.concatenate(update_terms, 0)
        rounded = reduced.astype(jnp.bfloat16)
        corrections[depth_k] = front_solve(tri_inverses, rounded, depth_k, False)
        parent_values = corrections[depth_k].astype(jnp.bfloat16)
    correction = jnp.stack([level_piece.reshape(NU // ROWS_DEV, SR, NRHS) for level_piece in corrections], 1).reshape(NU, NRHS)
    return solution + correction, residual
```

```python
import functools
import math

import jax
import jax.numpy as jnp
from jax import lax
from jax.experimental import pallas as pl
from jax.experimental.pallas import tpu as pltpu
from jax.sharding import PartitionSpec as P

MESH = pl.DeviceIdType.MESH
BF = jnp.bfloat16
F32 = jnp.float32
CORES = 2
SETS = 11


def sent_to_all(x, axis):
    copies = jnp.broadcast_to(x, (lax.axis_size(axis), *x.shape))
    return lax.all_to_all(copies, axis, split_axis=0, concat_axis=0, tiled=True)


def dot(a, b):
    return jnp.dot(a, b, preferred_element_type=F32)


def place_kernel(levels, spans, lower_ref, *refs):
    targets, out_ref, wide, placed = refs[:levels], refs[levels], refs[levels + 1], refs[levels + 2]
    tile = 256
    total = lower_ref.shape[0]

    @pl.loop(0, total // tile)
    def _(i):
        at = pl.ds(pl.multiple_of(i * tile, tile), tile)
        wide[at, :] = lower_ref[at, :].astype(F32)

    @pl.loop(0, 2 * total // tile)
    def _(i):
        at = pl.ds(pl.multiple_of(i * tile, tile), tile)
        placed[at, :] = jnp.zeros((tile, wide.shape[1]), F32)

    start = 0
    for level in range(levels):
        span = spans[level]
        step = 16

        @pl.loop(0, span // step)
        def _(i, level=level, start=start):
            for j in range(step):
                u = i * step + j
                to = targets[level][u]
                placed[pl.ds(2 * start + to, 1), :] = wide[pl.ds(start + u, 1), :]

        start += span

    rows = out_ref.shape[1]

    @pl.loop(0, out_ref.shape[0])
    def _(i):
        out_ref[i] = placed[pl.ds(pl.multiple_of(i * rows, rows), rows), :].astype(BF)


def place_rows(lower, targets):
    total, width = lower.shape
    spans = [t.shape[0] for t in targets]
    levels = len(spans)
    blocks = 2 * total // 128
    vmem = pl.BlockSpec(memory_space=pltpu.VMEM)
    smem = pl.BlockSpec(memory_space=pltpu.SMEM)
    return pl.pallas_call(
        functools.partial(place_kernel, levels, spans),
        out_shape=jax.ShapeDtypeStruct((blocks, 128, width), BF),
        in_specs=[vmem] + [smem] * levels,
        out_specs=vmem,
        scratch_shapes=[pltpu.VMEM((total, width), F32), pltpu.VMEM((2 * total, width), F32)],
        compiler_params=pltpu.CompilerParams(vmem_limit_bytes=56 * 2**20),
        cost_estimate=pl.CostEstimate(flops=10**10, bytes_accessed=10**7, transcendentals=0),
        name="place_rows",
    )(lower, *targets)


class Comm:
    def __init__(self, sizes, rows):
        self.axes = [a for a in ("x", "y", "z") if sizes[a] > 1]
        self.n = {a: sizes[a] for a in self.axes}
        if len(self.axes) == 2:
            a, b = self.axes
            half = rows // 2
            self.parts = [((a, b), 0, half), ((b, a), half, half)]
        else:
            third = rows * 3 // 8
            last = rows - 2 * third
            self.parts = [
                (("x", "y", "z"), 0, third),
                (("z", "x", "y"), third, third),
                (("y", "z", "x"), 2 * third, last),
            ]
        self.rows = rows

    def sum_parts(self):
        if len(self.axes) == 2:
            return self.parts
        third = self.rows * 3 // 8
        last = self.rows - 2 * third
        return [
            (("y", "z", "x"), 0, third),
            (("z", "x", "y"), third, third),
            (("x", "y", "z"), 2 * third, last),
        ]

    def sum_scratch(self):
        shapes = []
        for order, _, rows in self.sum_parts():
            left = list(self.axes)
            for j, a in enumerate(order):
                left.remove(a)
                dims = tuple(self.n[b] for b in left)
                shapes.append(pltpu.VMEM((self.n[a] - 1, *dims, rows, 128), BF))
                if j + 1 < len(order):
                    shapes.append(pltpu.VMEM((*dims, rows, 128), BF))
        return shapes


def main_kernel(cfg, *refs):
    names = cfg["names"]
    r = dict(zip(names, refs))
    levels, groups0, ny, nz, seg = cfg["levels"], cfg["groups0"], cfg["ny"], cfg["nz"], cfg["seg"]
    comms, comm_b = cfg["comms"], cfg["comm_b"]
    row = lax.axis_index("row")
    col = lax.axis_index("col")
    core = row % CORES
    other = 1 - core
    coord = {"x": row // CORES, "y": col // nz, "z": col % nz}
    size = {"x": cfg["nx"], "y": ny, "z": nz}
    plane = ny * nz * seg

    def device(axis, d, n):
        here = coord[axis]
        if axis == "x":
            base = here // n * n
            there = base + (here - base + d) % n
            return (there * CORES + core, col)
        there = (here + d) % n
        if axis == "y":
            return (row, there * nz + coord["z"])
        return (row, coord["y"] * nz + there)

    partner = (row + 1 - 2 * core, col)

    barrier = pltpu.get_barrier_semaphore()
    peers = [partner]
    for a in ("x", "y", "z"):
        peers += [device(a, d, size[a]) for d in range(1, size[a])]
    for peer in peers:
        pl.semaphore_signal(barrier, inc=1, device_id=peer, device_id_type=MESH)

    load = r["load_sem"]
    get_a = pltpu.make_async_copy(r["blocks"], r["al"], load.at[0])
    get_a.start()
    get_p = pltpu.make_async_copy(r["tri"], r["tri_buf"], load.at[1])
    get_p.start()
    get_w = pltpu.make_async_copy(r["upper"], r["upper_buf"], load.at[2])
    get_w.start()

    per = r["rhs"].shape[0]
    lanes = lax.broadcasted_iota(jnp.int32, (per, per), 1)
    r["hot"][...] = jnp.where(lanes == r["order"][...], 1.0, 0.0).astype(BF)

    pl.semaphore_wait(barrier, len(peers))

    def remote(src, dst, s, t, to):
        return pltpu.make_async_remote_copy(
            src_ref=src, dst_ref=dst, send_sem=s, recv_sem=t, device_id=to, device_id_type=MESH
        )

    def reduce(comm, first, scratch, turn):
        bufs = iter(scratch)
        state = []
        for order, r0, rows in comm.sum_parts():
            state.append(dict(order=order, r0=r0, rows=rows, left=list(comm.axes), cur=None))
        local = {a: coord[a] % comm.n[a] for a in comm.axes}
        stages = []
        for p, st in enumerate(state):
            mine = []
            for j in range(len(st["order"])):
                recv = next(bufs)
                nxt = next(bufs) if j + 1 < len(st["order"]) else None
                mine.append((recv, nxt))
            stages.append(mine)
        out = [None] * len(state)
        steps = len(state[0]["order"])

        def region(st, idx):
            if st["cur"] is None:
                return first(idx, pl.ds(st["r0"], st["rows"]))
            return st["cur"].at[tuple(idx)]

        def begin(p, j):
            st = state[p]
            a = st["order"][j]
            n = comm.n[a]
            pos = st["left"].index(a)
            copies = []
            for d in range(1, n):
                idx = [slice(None)] * len(st["left"])
                idx[pos] = (local[a] + d) % n
                c = remote(
                    region(st, idx),
                    stages[p][j][0].at[d - 1],
                    r["send_sem"].at[p, j, d - 1],
                    r["recv_sem"].at[turn, p, j, d - 1],
                    device(a, d, n),
                )
                c.start()
                copies.append(c)
            st["copies"] = copies

        def finish(p, j):
            st = state[p]
            a = st["order"][j]
            n = comm.n[a]
            pos = st["left"].index(a)
            for c in st["copies"]:
                c.wait_recv()
            recv, nxt = stages[p][j]
            rest = [b for b in st["left"] if b != a]
            dims = [comm.n[b] for b in rest]
            count = math.prod(dims)

            def total(at):
                idx = list(at)
                idx.insert(pos, local[a])
                value = region(st, idx)[...].astype(F32)
                for d in range(1, n):
                    value = value + recv[(d - 1, *at)].astype(F32)
                return value

            if nxt is None:
                out[p] = total([])
            elif len(dims) == 1:
                for i in range(dims[0]):
                    nxt[i] = total([i]).astype(BF)
            else:

                @pl.loop(0, count)
                def _(i):
                    at = [i // dims[1], i % dims[1]]
                    nxt[at[0], at[1]] = total(at).astype(BF)

            for c in st["copies"]:
                c.wait_send()
            st["left"] = rest
            st["cur"] = nxt

        for p in range(len(state)):
            begin(p, 0)
        for j in range(steps):
            for p in range(len(state)):
                finish(p, j)
                if j + 1 < steps:
                    begin(p, j + 1)
        return [(st["r0"], st["rows"], out[p]) for p, st in enumerate(state)]

    def gather(level, value, buf, turn):
        comm = comms[level]
        local = {a: coord[a] % comm.n[a] for a in comm.axes}
        here = {"x": local.get("x", 0), "y": coord["y"], "z": coord["z"]}

        def block(idx, c, rows):
            return buf.at[(idx["x"], c, idx["y"], idx["z"], rows)]

        every = pl.ds(0, seg)
        buf[here["x"], core, here["y"], here["z"]] = value
        d2d_send = r["d2d_send"].at[0]
        d2d_recv = r["d2d_recv"].at[turn]
        own = block(here, core, every)
        remote(own, own, d2d_send, d2d_recv, partner).start()
        pending = []

        def span(order, j, shift_axis=None, d=0):
            idx = dict(here)
            for a in order[:j]:
                idx[a] = slice(None)
            if shift_axis is not None:
                n = comm.n[shift_axis]
                idx[shift_axis] = (local[shift_axis] + n - d) % n
            return idx

        def begin(p, j):
            order, r0, rows = comm.parts[p]
            a = order[j]
            n = comm.n[a]
            src = block(span(order, j), core, pl.ds(r0, rows))
            for d in range(1, n):
                c = remote(
                    src,
                    src,
                    r["send_sem"].at[p, j, d - 1],
                    r["recv_sem"].at[turn, p, j, d - 1],
                    device(a, d, n),
                )
                c.start()
                pending.append(c)

        def finish(p, j):
            order, r0, rows = comm.parts[p]
            a = order[j]
            n = comm.n[a]
            for d in range(1, n):
                got = block(span(order, j, a, d), core, pl.ds(r0, rows))
                remote(
                    got,
                    got,
                    r["send_sem"].at[p, j, d - 1],
                    r["recv_sem"].at[turn, p, j, d - 1],
                    device(a, d, n),
                ).wait_recv()
                remote(got, got, d2d_send, d2d_recv, partner).start()

        steps = len(comm.axes)
        for p in range(len(comm.parts)):
            begin(p, 0)
        for j in range(steps):
            for p in range(len(comm.parts)):
                finish(p, j)
                if j + 1 < steps:
                    begin(p, j + 1)
        for c in pending:
            c.wait_send()
        mine, theirs = buf.at[:, core], buf.at[:, other]
        remote(mine, theirs, d2d_send, d2d_recv, partner).wait()

    offsets = cfg["offsets"]

    def triangle(level, buf, lower):
        off = offsets[level]
        fronts = groups0 * 2**level
        me = row % fronts

        def panel(g):
            return r["tri_buf"][:, pl.ds(pl.multiple_of(off + g * plane, 128), plane)]

        def vector(g):
            return buf[g // CORES, g % CORES].reshape(plane, 128)

        row_ids = col * seg + lax.broadcasted_iota(jnp.int32, (seg, plane), 0)
        col_ids = lax.broadcasted_iota(jnp.int32, (seg, plane), 1)
        keep = col_ids < row_ids if lower else col_ids >= row_ids
        masked = jnp.where(keep, panel(me).astype(F32), 0.0).astype(BF)
        acc = dot(masked, vector(me))

        def more(g, acc):
            return acc + dot(panel(g), vector(g))

        if lower:
            return lax.fori_loop(0, me, more, acc)
        return lax.fori_loop(me + 1, fronts, more, acc)

    get_a.wait()
    al, sol, tb = r["al"], r["gathered"], r["tb"]
    kb = cfg["kb"]
    bpd = per // 128

    @pl.loop(0, ny * nz)
    def _(c):
        for j in range(bpd):
            i = c * bpd + j
            left = jnp.concatenate([al[i * kb + s] for s in range(kb)], 1)
            right = jnp.concatenate(
                [sol[r["where"][i * kb + s]] for s in range(kb)], 0
            )
            tb[c // nz, c % nz, j * 128 : (j + 1) * 128, :] = dot(left, right).astype(BF)

    get_l = pltpu.make_async_copy(r["placed"], al, load.at[0])
    get_l.start()

    def first_b(idx, rows):
        return tb.at[(*idx, rows)]

    for r0, rows, value in reduce(comm_b, first_b, r["sum_b"], 0):
        at = slice(r0, r0 + rows)
        res = r["rhs"][at, :] - value
        r["residual"][at, :] = res
        hi = res.astype(BF)
        r["split"][at, 0:128] = hi
        r["split"][at, 128:256] = (res - hi.astype(F32)).astype(BF)
    both = dot(r["hot"][...], r["split"][...])
    r["vee"][...] = both[:, 0:128] + both[:, 128:256]

    get_p.wait()
    turn = 1
    buf_a, buf_b = r["buf_a"], r["buf_b"]
    incoming = None
    for level in range(levels):
        e = r["vee"][level * seg : (level + 1) * seg, :]
        if level > 0:
            parts = incoming
            for r0, rows, value in parts:
                r["minus"][r0 : r0 + rows, :] = value
            e = e - r["minus"][...]
        cb = e.astype(BF)
        gather(level, cb, buf_a[level], turn % SETS)
        turn += 1
        y = (triangle(level, buf_a[level], True) + cb.astype(F32)).astype(BF)
        r["why"][level] = y
        if level == 0:
            get_l.wait()
        if level + 1 < levels:
            t, rd = r["t"][level], r["rd"][level]
            nx = t.shape[0]
            base = 2 * offsets[level] // 128
            half = ny // 2
            per_half = half * nz

            def update(xi, ci, level=level, t=t, base=base, y=y):
                for h in range(2):
                    at = base + (xi * CORES + ci) * (ny * nz) + h * per_half
                    block = al[pl.ds(at, per_half)].reshape(per_half * 128, 128)
                    res = dot(block, y).astype(BF)
                    t[xi, ci, h * half : (h + 1) * half] = res.reshape(half, nz, 128, 128)

            d2d_send, d2d_recv = r["d2d_send"].at[0], r["d2d_recv"].at[turn % SETS]
            for xi in range(nx):
                update(xi, other)
                remote(t.at[xi, other], rd.at[xi], d2d_send, d2d_recv, partner).start()
            for xi in range(nx):
                update(xi, core)
            remote(t.at[:, other], rd, d2d_send, d2d_recv, partner).wait()

            @pl.loop(0, nx * ny)
            def _(i, t=t, rd=rd):
                xi, yi = i // ny, i % ny
                for zi in range(nz):
                    value = t[xi, core, yi, zi].astype(F32) + rd[xi, yi, zi].astype(F32)
                    t[xi, core, yi, zi] = value.astype(BF)

            def first(idx, rows, t=t):
                return t.at[(idx[0], core, idx[1], idx[2], rows)]

            incoming = reduce(comms[level + 1], first, r["sums"][level], turn % SETS)
            turn += 1

    get_w.wait()
    xb = None
    for level in reversed(range(levels)):
        z = r["why"][level]
        if level + 1 < levels:
            src = buf_a[level + 1]
            wide, picked = r["wide"], r["picked"]
            xs = src.shape[0]

            @pl.loop(0, xs * CORES * ny)
            def _(i, src=src):
                xi, ci, yi = i // (CORES * ny), i // ny % CORES, i % ny
                block = src[xi, ci, yi].reshape(nz * 128, 128)
                wide[pl.ds(pl.multiple_of(i * nz * 128, 128), nz * 128), :] = block.astype(F32)

            m = offsets[level + 1] - offsets[level]
            tile = picked.shape[0]
            where = r["targets"][level]
            step = 16

            def chunk(i, acc, level=level, where=where):
                @pl.loop(0, tile // step)
                def _(u):
                    for v in range(step):
                        w = u * step + v
                        picked[w] = wide[where[i * tile + w]]

                at = pl.ds(pl.multiple_of(offsets[level] + i * tile, 128), tile)
                return acc + dot(r["upper_buf"][:, at], picked[...].astype(BF))

            total = lax.fori_loop(0, m // tile, chunk, jnp.zeros((seg, 128), F32))
            z = (z.astype(F32) - total).astype(BF)
        gather(level, z, buf_b[level], turn % SETS)
        turn += 1
        x = triangle(level, buf_b[level], False)
        at = slice(level * seg, (level + 1) * seg)
        r["refined"][at, :] = r["old"][at, :] + x
        if level > 0:
            gather(level, x.astype(BF), buf_a[level], turn % SETS)
            turn += 1


def refine(nx, ny, nz, gathered, solution, rhs, blocks, where, order, tri, placed, upper, targets):
    per = rhs.shape[0]
    levels = len(targets) + 1
    seg = per // levels
    cols = ny * nz
    groups0 = CORES
    span0 = groups0 * cols * seg
    offsets = [span0 * (2**k - 1) for k in range(levels + 1)]
    comms = [Comm({"x": 2**k, "y": ny, "z": nz}, seg) for k in range(levels)]
    comm_b = Comm({"x": 1, "y": ny, "z": nz}, per)
    vmem = pl.BlockSpec(memory_space=pltpu.VMEM)
    smem = pl.BlockSpec(memory_space=pltpu.SMEM)
    hbm = pl.BlockSpec(memory_space=pl.ANY)
    ins = [
        ("gathered", vmem), ("old", vmem), ("rhs", vmem), ("blocks", hbm), ("where", smem), ("order", vmem),
        ("tri", hbm), ("placed", hbm), ("upper", hbm),
    ]
    names = [n for n, _ in ins] + [f"target{k}" for k in range(levels - 1)]
    in_specs = [s for _, s in ins] + [smem] * (levels - 1)
    names += ["refined", "residual"]
    front = lambda k: (2**k, CORES, ny, nz, seg, 128)
    scratch = {
        "al": pltpu.VMEM(blocks.shape, BF),
        "tri_buf": pltpu.VMEM(tri.shape, BF),
        "upper_buf": pltpu.VMEM(upper.shape, BF),
        "hot": pltpu.VMEM((per, per), BF),
        "tb": pltpu.VMEM((ny, nz, per, 128), BF),
        "split": pltpu.VMEM((per, 256), BF),
        "vee": pltpu.VMEM((per, 128), F32),
        "minus": pltpu.VMEM((seg, 128), F32),
        "why": pltpu.VMEM((levels, seg, 128), BF),
        "wide": pltpu.VMEM((2 ** (levels - 1) * span0, 128), F32),
        "picked": pltpu.VMEM((1024, 128), F32),
        "load_sem": pltpu.SemaphoreType.DMA((3,)),
        "send_sem": pltpu.SemaphoreType.DMA((3, 3, 3)),
        "recv_sem": pltpu.SemaphoreType.DMA((SETS, 3, 3, 3)),
        "d2d_send": pltpu.SemaphoreType.DMA((1,)),
        "d2d_recv": pltpu.SemaphoreType.DMA((SETS,)),
    }
    names += list(scratch)
    shapes = list(scratch.values())
    lists = {
        "buf_a": [pltpu.VMEM(front(k), BF) for k in range(levels)],
        "buf_b": [pltpu.VMEM(front(k), BF) for k in range(levels)],
        "t": [pltpu.VMEM(front(k + 1), BF) for k in range(levels - 1)],
        "rd": [pltpu.VMEM((2 ** (k + 1), ny, nz, seg, 128), BF) for k in range(levels - 1)],
        "sum_b": comm_b.sum_scratch(),
    }
    for k in range(levels - 1):
        lists[f"sums{k}"] = comms[k + 1].sum_scratch()
    for name, items in lists.items():
        names += [f"{name}.{i}" for i in range(len(items))]
        shapes += items

    def body(*refs):
        flat = dict(zip(names, refs))
        r = {n: v for n, v in flat.items() if "." not in n}
        for name, items in lists.items():
            r[name] = [flat[f"{name}.{i}"] for i in range(len(items))]
        r["sums"] = [r[f"sums{k}"] for k in range(levels - 1)]
        r["targets"] = [r[f"target{k}"] for k in range(levels - 1)]
        cfg = dict(
            names=list(r), levels=levels, groups0=groups0, nx=nx, ny=ny, nz=nz, seg=seg,
            comms=comms, comm_b=comm_b, offsets=offsets, kb=where.shape[0] // (cols * per // 128),
        )
        main_kernel(cfg, *r.values())

    return pl.pallas_call(
        body,
        out_shape=(jax.ShapeDtypeStruct(rhs.shape, F32), jax.ShapeDtypeStruct(rhs.shape, F32)),
        in_specs=in_specs,
        out_specs=(vmem, vmem),
        scratch_shapes=shapes,
        compiler_params=pltpu.CompilerParams(
            collective_id=0, has_side_effects=True, vmem_limit_bytes=67043328
        ),
        cost_estimate=pl.CostEstimate(flops=10**10, bytes_accessed=3 * 10**7, transcendentals=0),
        name="refine_step",
    )(gathered, solution, rhs, blocks, where, order, tri, placed, upper, *targets)


def on_device(
    solution,
    right_side,
    block_values,
    block_columns,
    row_order,
    tri_inverses,
    lower_updates,
    upper_updates,
    update_rows,
):
    row_count = lax.axis_size("row")
    col_count = lax.axis_size("col")
    levels = row_count.bit_length() - 1
    per = solution.shape[0]
    seg = per // levels
    block_size = block_values.shape[2]
    per_block = per // block_size
    row_index = lax.axis_index("row")
    col_index = lax.axis_index("col")
    span0 = CORES * col_count * seg
    gathered = sent_to_all(solution.astype(BF), "row").reshape(row_count * per_block, block_size, -1)
    targets = []
    for k in range(levels - 1):
        span = span0 * 2**k
        front = row_index // 2 ** (k + 1)
        targets.append(lax.dynamic_slice_in_dim(update_rows[k], front * span, span))
    placed = place_rows(lower_updates, targets)
    local_block = block_columns // (per_block * col_count) * per_block + block_columns % per_block
    order = row_order - (row_index * col_count + col_index) * per
    ny = math.isqrt(col_count)
    return refine(
        row_count // CORES,
        ny,
        col_count // ny,
        gathered,
        solution,
        right_side,
        block_values.reshape(-1, block_size, block_size),
        local_block.reshape(-1),
        order.reshape(-1, 1),
        tri_inverses,
        placed,
        upper_updates,
        targets,
    )


def solution(mesh):
    in_specs = (
        P(("row", "col"), None),
        P(("row", "col"), None),
        P("row", "col", None, None),
        P("row", "col"),
        P(("row", "col")),
        P(("row", "col"), None),
        P(None, ("row", "col")),
        P(("row", "col"), None),
        P(),
    )
    out_specs = (P(("row", "col"), None), P(("row", "col"), None))
    return jax.shard_map(
        on_device, mesh=mesh, in_specs=in_specs, out_specs=out_specs, check_vma=False
    )
```

```python
import functools
import math

import jax
import jax.numpy as jnp
from jax import lax
from jax.experimental import pallas as pl
from jax.experimental.pallas import tpu as pltpu
from jax.sharding import PartitionSpec as P

MESH = pl.DeviceIdType.MESH
BF = jnp.bfloat16
F32 = jnp.float32
CORES = 2


def sent_to_all(x, axis):
    copies = jnp.broadcast_to(x, (lax.axis_size(axis), *x.shape))
    return lax.all_to_all(copies, axis, split_axis=0, concat_axis=0, tiled=True)


def dot(a, b):
    return jnp.dot(a, b, preferred_element_type=F32)


def place_kernel(spans, lower, updates, out, narrow, wide, placed, done, where, sem_in, sem_out, sem_idx):
    rows = 256
    step = 32
    row = lax.axis_index("row")
    copies = []
    start = 0
    for level, span in enumerate(spans):
        at = pl.ds(start, span)
        front = pl.multiple_of(level * (updates.shape[0] // len(spans)) + row // 2 ** (level + 1) * span, 1024)
        idx = pltpu.make_async_copy(updates.at[pl.ds(front, span)], where.at[at], sem_idx.at[level])
        idx.start()
        got = pltpu.make_async_copy(lower.at[at], narrow.at[at], sem_in.at[level])
        got.start()
        copies.append((idx, got))
        start += span

    start = 0
    puts = []
    for level, span in enumerate(spans):

        @pl.loop(0, 2 * span // rows)
        def _(i, start=start):
            at = pl.multiple_of(2 * start + i * rows, rows)
            placed[pl.ds(at, rows), :] = jnp.zeros((rows, placed.shape[1]), F32)

        for copy in copies[level]:
            copy.wait()

        @pl.loop(0, span // rows)
        def _(i, start=start):
            at = pl.ds(pl.multiple_of(start + i * rows, rows), rows)
            wide[at, :] = narrow[at, :].astype(F32)

        @pl.loop(0, span // step)
        def _(i, start=start):
            for j in range(step):
                u = start + i * step + j
                placed[2 * start + where[u]] = wide[u]

        block = out.shape[1]
        for part in range(2):
            first = (2 * start + part * span) // block

            @pl.loop(first, first + span // block)
            def _(i):
                done[i] = placed[pl.ds(pl.multiple_of(i * block, block), block), :].astype(BF)

            at = pl.ds(first, span // block)
            put = pltpu.make_async_copy(done.at[at], out.at[at], sem_out.at[level, part])
            put.start()
            puts.append(put)
        start += span
    for put in puts:
        put.wait()


def place_rows(lower, updates, spans):
    total, width = lower.shape
    blocks = 2 * total // 128
    hbm = pl.BlockSpec(memory_space=pl.ANY)
    return pl.pallas_call(
        functools.partial(place_kernel, spans),
        out_shape=jax.ShapeDtypeStruct((blocks, 128, width), BF),
        in_specs=[hbm, hbm],
        out_specs=hbm,
        scratch_shapes=[
            pltpu.VMEM((total, width), BF),
            pltpu.VMEM((total, width), F32),
            pltpu.VMEM((2 * total, width), F32),
            pltpu.VMEM((blocks, 128, width), BF),
            pltpu.SMEM((total,), jnp.int32),
            pltpu.SemaphoreType.DMA((len(spans),)),
            pltpu.SemaphoreType.DMA((len(spans), 2)),
            pltpu.SemaphoreType.DMA((len(spans),)),
        ],
        compiler_params=pltpu.CompilerParams(vmem_limit_bytes=56 * 2**20),
        cost_estimate=pl.CostEstimate(flops=10**10, bytes_accessed=10**7, transcendentals=0),
        name="place_rows",
    )(lower, updates)


class Comm:
    def __init__(self, sizes, rows):
        self.axes = [a for a in ("x", "y", "z") if sizes[a] > 1]
        self.n = {a: sizes[a] for a in self.axes}
        if len(self.axes) == 2:
            a, b = self.axes
            half = rows // 2
            self.parts = [((a, b), 0, half), ((b, a), half, half)]
        else:
            third = rows * 3 // 8
            self.parts = [
                (("x", "y", "z"), 0, third),
                (("z", "x", "y"), third, third),
                (("y", "z", "x"), 2 * third, rows - 2 * third),
            ]
        self.rows = rows
        steps = len(self.axes)
        self.messages = [(j, mask) for j in range(steps) for mask in range(2**j)]
        self.blocks = math.prod(self.n.values())

    def span(self, order, mask, at):
        index = {}
        for i, a in enumerate(order):
            index[a] = slice(1, self.n[a]) if mask >> i & 1 else at.get(a, 0)
        return index

    def sum_scratch(self):
        shapes = []
        for order, _, rows in self.parts:
            for j, mask in self.messages:
                dims = [self.n[a] - 1 for a in self.axes if mask >> order.index(a) & 1]
                shapes.append(pltpu.VMEM((self.n[order[j]] - 1, *dims, rows, 128), BF))
        return shapes


def main_kernel(cfg, *refs):
    names = cfg["names"]
    r = dict(zip(names, refs))
    levels, groups0, ny, nz, seg = cfg["levels"], cfg["groups0"], cfg["ny"], cfg["nz"], cfg["seg"]
    comms, comm_b = cfg["comms"], cfg["comm_b"]
    row = lax.axis_index("row")
    col = lax.axis_index("col")
    core = row % CORES
    other = 1 - core
    coord = {"x": row // CORES, "y": col // nz, "z": col % nz}
    size = {"x": cfg["nx"], "y": ny, "z": nz}
    plane = ny * nz * seg

    def device(axis, d, n):
        here = coord[axis]
        if axis == "x":
            base = here // n * n
            there = base + (here - base + d) % n
            return (there * CORES + core, col)
        there = (here + d) % n
        if axis == "y":
            return (row, there * nz + coord["z"])
        return (row, coord["y"] * nz + there)

    partner = (row + 1 - 2 * core, col)

    barrier = pltpu.get_barrier_semaphore()
    peers = [partner]
    for a in ("x", "y", "z"):
        peers += [device(a, d, size[a]) for d in range(1, size[a])]
    for peer in peers:
        pl.semaphore_signal(barrier, inc=1, device_id=peer, device_id_type=MESH)

    load = r["load_sem"]
    get_a = pltpu.make_async_copy(r["blocks"], r["al"], load.at[0])
    get_a.start()
    get_p = pltpu.make_async_copy(r["tri"], r["tri_buf"], load.at[1])
    get_w = pltpu.make_async_copy(r["upper"], r["upper_buf"], load.at[2])

    per = r["rhs"].shape[0]
    source = lax.broadcasted_iota(jnp.int32, (per, per), 0) + (row * ny * nz + col) * per
    to = jnp.broadcast_to(r["order"][...].reshape(1, per), (per, per))
    r["hot"][...] = jnp.where(source == to, 1.0, 0.0).T.astype(BF)

    pl.semaphore_wait(barrier, len(peers))

    def remote(src, dst, s, t, to):
        return pltpu.make_async_remote_copy(
            src_ref=src, dst_ref=dst, send_sem=s, recv_sem=t, device_id=to, device_id_type=MESH
        )

    def reduce(comm, ref, scratch, turn):
        steps = len(comm.axes)
        count = len(comm.messages)
        slot = {m: i for i, m in enumerate(comm.messages)}
        recv = [scratch[p * count : (p + 1) * count] for p in range(len(comm.parts))]
        sends = r["send_sem"].at[turn]
        full = (1 << steps) - 1

        def copy(p, j, mask, d):
            order, r0, rows = comm.parts[p]
            a = order[j]
            index = comm.span(order, mask, {a: d})
            return remote(
                ref(index, pl.ds(r0, rows)),
                recv[p][slot[j, mask]].at[d - 1],
                sends,
                r["recv_sem"].at[turn, p, slot[j, mask]],
                device(a, d, comm.n[a]),
            )

        def send(p, j, mask):
            for d in range(1, comm.n[comm.parts[p][0][j]]):
                copy(p, j, mask, d).start()

        arrived = set()

        def wait(p, j, mask):
            if (p, j, mask) not in arrived:
                arrived.add((p, j, mask))
                buf = recv[p][slot[j, mask]]
                sem = r["recv_sem"].at[turn, p, slot[j, mask]]
                remote(buf, buf, sends, sem, partner).wait_recv()

        def total(p, mask, low):
            order, r0, rows = comm.parts[p]
            froms = [recv[p][slot[j, mask]] for j in range(low, steps)]
            for j in range(low, steps):
                wait(p, j, mask)
            axes = [a for a in comm.axes if mask >> order.index(a) & 1]
            dims = [comm.n[a] - 1 for a in axes]

            def one(at):
                index = {a: 0 for a in order}
                for a, where in zip(axes, at):
                    index[a] = where + 1
                here = ref(index, pl.ds(r0, rows))
                value = here[...].astype(F32)
                for buf in froms:
                    for d in range(buf.shape[0]):
                        value = value + buf[(d, *at)].astype(F32)
                return here, value

            if not axes:
                return one(())[1]
            if len(dims) == 1:
                for i in range(dims[0]):
                    here, value = one((i,))
                    here[...] = value.astype(BF)
            else:

                @pl.loop(0, dims[0])
                def _(i):
                    for k in range(dims[1]):
                        here, value = one((i, k))
                        here[...] = value.astype(BF)

        parts = range(len(comm.parts))
        last = steps - 1
        order_of = sorted(range(2**last), key=lambda m: -bin(m).count("1"))
        for mask in order_of:
            for p in parts:
                send(p, last, mask)
        for i in reversed(range(last)):
            for mask in sorted(range(2**i), key=lambda m: -bin(m).count("1")):
                for p in parts:
                    total(p, mask | 1 << i, i + 1)
                    send(p, i, mask)
        out = [total(p, 0, 0) for p in parts]
        sent = sum((comm.blocks - 1) * rows for _, _, rows in comm.parts)
        everything = drain(sent)
        remote(everything, everything, sends, r["recv_sem"].at[turn, 0, 0], partner).wait_send()
        return [(r0, rows, out[p]) for p, (_, r0, rows) in enumerate(comm.parts)]

    def drain(rows):
        return r["al"].at[pl.ds(0, rows // 128)]

    def gather(level, value, buf, turn):
        comm = comms[level]
        steps = len(comm.axes)
        slot = {m: i for i, m in enumerate(comm.messages)}
        sends = r["send_sem"].at[turn]
        d2d_send = r["d2d_send"].at[turn]
        d2d_recv = r["d2d_recv"].at[turn]

        def block(index, side, rows):
            return buf.at[(index.get("x", 0), side, index["y"], index["z"], rows)]

        buf[0, 0, 0, 0] = value

        def send(p, j, mask):
            order, r0, rows = comm.parts[p]
            a = order[j]
            n = comm.n[a]
            src = block(comm.span(order, mask, {}), 0, pl.ds(r0, rows))
            for d in range(1, n):
                dst = block(comm.span(order, mask, {a: n - d}), 0, pl.ds(r0, rows))
                remote(src, dst, sends, r["recv_sem"].at[turn, p, slot[j, mask]], device(a, d, n)).start()

        def arrive(p, j, mask):
            order, r0, rows = comm.parts[p]
            index = comm.span(order, mask | 1 << j, {})
            got = block(index, 0, pl.ds(r0, rows))
            remote(got, got, sends, r["recv_sem"].at[turn, p, slot[j, mask]], partner).wait_recv()
            for k in range(j + 1, steps):
                send(p, k, mask | 1 << j)
            remote(got, block(index, 1, pl.ds(r0, rows)), d2d_send, d2d_recv, partner).start()

        parts = range(len(comm.parts))
        for j in range(steps):
            for p in parts:
                send(p, j, 0)
        remote(buf.at[0, 0, 0, 0], buf.at[0, 1, 0, 0], d2d_send, d2d_recv, partner).start()
        for j, mask in sorted(comm.messages, key=lambda m: (bin(m[1]).count("1"), m[0])):
            for p in parts:
                arrive(p, j, mask)
        sent = sum((comm.blocks - 1) * rows for _, _, rows in comm.parts)
        everything = drain(sent)
        remote(everything, everything, sends, r["recv_sem"].at[turn, 0, 0], partner).wait_send()
        remote(buf.at[:, 0], buf.at[:, 1], d2d_send, d2d_recv, partner).wait()

    offsets = cfg["offsets"]
    natural = [
        ((yi + ny - coord["y"]) % ny, (zi + nz - coord["z"]) % nz) for yi in range(ny) for zi in range(nz)
    ]

    def place(nx, dx, side, dy, dz):
        xi = (coord["x"] % nx + dx) % nx
        ci = (core + side) % CORES
        return ((xi * CORES + ci) * ny + (coord["y"] + dy) % ny) * nz + (coord["z"] + dz) % nz

    def triangle(level, buf, lower):
        off = offsets[level]
        fronts = groups0 * 2**level
        me = row % fronts

        def panel(g):
            return r["tri_buf"][:, pl.ds(pl.multiple_of(off + g * plane, 128), plane)]

        nx = buf.shape[0]

        def vector(g):
            dx = (g // CORES + nx - coord["x"] % nx) % nx
            side = (g + core) % CORES
            return jnp.concatenate([buf[dx, side, dy, dz] for dy, dz in natural], 0)

        row_ids = col * seg + lax.broadcasted_iota(jnp.int32, (seg, plane), 0)
        col_ids = lax.broadcasted_iota(jnp.int32, (seg, plane), 1)
        keep = col_ids < row_ids if lower else col_ids >= row_ids
        masked = jnp.where(keep, panel(me).astype(F32), 0.0).astype(BF)
        acc = dot(masked, vector(me))

        def more(g, acc):
            return acc + dot(panel(g), vector(g))

        if lower:
            return lax.fori_loop(0, me, more, acc)
        return lax.fori_loop(me + 1, fronts, more, acc)

    get_idx = []
    for k in range(levels - 1):
        m = cfg["offsets"][k + 1] - cfg["offsets"][k]
        first = pl.multiple_of(k * (r["updates"].shape[0] // (levels - 1)) + row // 2 ** (k + 1) * m, 1024)
        at = pl.ds(cfg["offsets"][k], m)
        get_idx.append(pltpu.make_async_copy(r["updates"].at[pl.ds(first, m)], r["targets"].at[at], load.at[3 + k]))
    get_a.wait()
    for copy in (get_p, get_w, *get_idx):
        copy.start()
    al, sol, tb = r["al"], r["gathered"], r["tb"]
    kb = r["where"].shape[1]
    bpd = per // 128
    group = bpd * ny * nz

    def block_at(i, s):
        b = r["where"][i, s]
        return sol[b // group * bpd + b % bpd]

    @pl.loop(0, ny * nz)
    def _(c):
        dy, dz = c // nz, c % nz
        to = (coord["y"] + dy) % ny * nz + (coord["z"] + dz) % nz
        for j in range(bpd):
            i = to * bpd + j
            left = jnp.concatenate([al[i * kb + s] for s in range(kb)], 1)
            right = jnp.concatenate([block_at(i, s) for s in range(kb)], 0)
            tb[dy, dz, j * 128 : (j + 1) * 128, :] = dot(left, right).astype(BF)

    get_l = pltpu.make_async_copy(r["placed"], al, load.at[0])
    get_l.start()

    def first_b(index, rows):
        return tb.at[(index["y"], index["z"], rows)]

    for r0, rows, value in reduce(comm_b, first_b, r["sum_b"], 0):
        at = slice(r0, r0 + rows)
        r["product"][at, :] = value
        res = r["rhs"][at, :] - value
        hi = res.astype(BF)
        r["split"][at, 0:128] = hi
        r["split"][at, 128:256] = (res - hi.astype(F32)).astype(BF)
    both = dot(r["hot"][...], r["split"][...])
    r["vee"][...] = both[:, 0:128] + both[:, 128:256]

    get_p.wait()
    turn = 1
    buf_a, buf_b = r["buf_a"], r["buf_b"]
    incoming = None
    for level in range(levels):
        e = r["vee"][level * seg : (level + 1) * seg, :]
        if level > 0:
            parts = incoming
            for r0, rows, value in parts:
                r["minus"][r0 : r0 + rows, :] = value
            e = e - r["minus"][...]
        cb = e.astype(BF)
        gather(level, cb, buf_a[level], turn)
        turn += 1
        y = (triangle(level, buf_a[level], True) + cb.astype(F32)).astype(BF)
        r["why"][level] = y
        if level == 0:
            get_l.wait()
        if level + 1 < levels:
            t, rd = r["t"][level], r["rd"][level]
            nx = t.shape[0]
            base = 2 * offsets[level] // 128
            half = ny // 2

            def update(dx, side, t=t, base=base, y=y, nx=nx):
                for h in range(2):
                    spots = [(dy, dz) for dy in range(h * half, (h + 1) * half) for dz in range(nz)]
                    rows = [al[base + place(nx, dx, side, dy, dz)] for dy, dz in spots]
                    res = dot(jnp.concatenate(rows, 0), y).astype(BF)
                    t[dx, side, h * half : (h + 1) * half] = res.reshape(half, nz, 128, 128)

            d2d_send, d2d_recv = r["d2d_send"].at[turn], r["d2d_recv"].at[turn]
            for xi in range(nx):
                update(xi, 1)
                remote(t.at[xi, 1], rd.at[xi], d2d_send, d2d_recv, partner).start()
            for xi in range(nx):
                update(xi, 0)
            remote(t.at[:, 1], rd, d2d_send, d2d_recv, partner).wait()

            @pl.loop(0, nx * ny)
            def _(i, t=t, rd=rd):
                xi, yi = i // ny, i % ny
                for zi in range(nz):
                    value = t[xi, 0, yi, zi].astype(F32) + rd[xi, yi, zi].astype(F32)
                    t[xi, 0, yi, zi] = value.astype(BF)

            def first(index, rows, t=t):
                return t.at[(index["x"], 0, index["y"], index["z"], rows)]

            incoming = reduce(comms[level + 1], first, r["sums"][level], turn)
            turn += 1

    for copy in (get_w, *get_idx):
        copy.wait()
    xb = None
    for level in reversed(range(levels)):
        z = r["why"][level]
        if level + 1 < levels:
            src = buf_a[level + 1]
            wide, picked = r["wide"], r["picked"]
            xs = src.shape[0]

            @pl.loop(0, xs * CORES * ny)
            def _(i, src=src, xs=xs):
                dx, side, dy = i // (CORES * ny), i // ny % CORES, i % ny
                for dz in range(nz):
                    to = pl.multiple_of(place(xs, dx, side, dy, dz) * 128, 128)
                    wide[pl.ds(to, 128), :] = src[dx, side, dy, dz].astype(F32)

            m = offsets[level + 1] - offsets[level]
            tile = picked.shape[0]
            tiles = m // tile // CORES
            where = r["targets"]
            step = 32
            rows = r["rows"]
            d2d_send, d2d_recv = r["d2d_send"].at[turn], r["d2d_recv"].at[turn]

            def product(i, acc, level=level):
                at = pl.ds(pl.multiple_of(offsets[level] + i * tile, 128), tile)
                return acc + dot(r["upper_buf"][:, at], rows[i])

            def chunk(i, acc, level=level, tiles=tiles):
                mine = core * tiles + i
                first = offsets[level] + mine * tile

                @pl.loop(0, tile // step)
                def _(u):
                    for v in range(step):
                        w = u * step + v
                        picked[w] = wide[where[first + w]]

                rows[mine] = picked[...].astype(BF)
                remote(rows.at[mine], rows.at[mine], d2d_send, d2d_recv, partner).start()
                return product(mine, acc)

            total = lax.fori_loop(0, tiles, chunk, jnp.zeros((seg, 128), F32))
            sent, got = rows.at[pl.ds(core * tiles, tiles)], rows.at[pl.ds(other * tiles, tiles)]
            remote(sent, got, d2d_send, d2d_recv, partner).wait()
            total = lax.fori_loop(other * tiles, (other + 1) * tiles, product, total)
            turn += 1
            z = (z.astype(F32) - total).astype(BF)
        gather(level, z, buf_b[level], turn)
        turn += 1
        x = triangle(level, buf_b[level], False)
        at = slice(level * seg, (level + 1) * seg)
        r["correction"][at, :] = x
        if level > 0:
            gather(level, x.astype(BF), buf_a[level], turn)
            turn += 1


def refine(levels, nx, ny, nz, gathered, rhs, blocks, where, order, tri, placed, upper, updates):
    per = rhs.shape[0]
    seg = per // levels
    cols = ny * nz
    groups0 = CORES
    span0 = groups0 * cols * seg
    offsets = [span0 * (2**k - 1) for k in range(levels + 1)]
    comms = [Comm({"x": 2**k, "y": ny, "z": nz}, seg) for k in range(levels)]
    comm_b = Comm({"x": 1, "y": ny, "z": nz}, per)
    turns = 5 * levels - 2
    vmem = pl.BlockSpec(memory_space=pltpu.VMEM)
    smem = pl.BlockSpec(memory_space=pltpu.SMEM)
    hbm = pl.BlockSpec(memory_space=pl.ANY)
    ins = [
        ("gathered", vmem), ("rhs", vmem), ("blocks", hbm), ("where", smem), ("order", vmem),
        ("tri", hbm), ("placed", hbm), ("upper", hbm), ("updates", hbm),
    ]
    names = [n for n, _ in ins]
    in_specs = [s for _, s in ins]
    names += ["correction", "product"]
    front = lambda k: (2**k, CORES, ny, nz, seg, 128)
    scratch = {
        "al": pltpu.VMEM(blocks.shape, BF),
        "tri_buf": pltpu.VMEM(tri.shape, BF),
        "upper_buf": pltpu.VMEM(upper.shape, BF),
        "hot": pltpu.VMEM((per, per), BF),
        "tb": pltpu.VMEM((ny, nz, per, 128), BF),
        "split": pltpu.VMEM((per, 256), BF),
        "vee": pltpu.VMEM((per, 128), F32),
        "minus": pltpu.VMEM((seg, 128), F32),
        "why": pltpu.VMEM((levels, seg, 128), BF),
        "wide": pltpu.VMEM((2 ** (levels - 1) * span0, 128), F32),
        "picked": pltpu.VMEM((1024, 128), F32),
        "rows": pltpu.VMEM(((offsets[levels - 1] - offsets[levels - 2]) // 1024, 1024, 128), BF),
        "targets": pltpu.SMEM((offsets[levels - 1],), jnp.int32),
        "load_sem": pltpu.SemaphoreType.DMA((2 + levels,)),
        "send_sem": pltpu.SemaphoreType.DMA((turns,)),
        "recv_sem": pltpu.SemaphoreType.DMA((turns, 3, 7)),
        "d2d_send": pltpu.SemaphoreType.DMA((turns,)),
        "d2d_recv": pltpu.SemaphoreType.DMA((turns,)),
    }
    names += list(scratch)
    shapes = list(scratch.values())
    lists = {
        "buf_a": [pltpu.VMEM(front(k), BF) for k in range(levels)],
        "buf_b": [pltpu.VMEM(front(k), BF) for k in range(levels)],
        "t": [pltpu.VMEM(front(k + 1), BF) for k in range(levels - 1)],
        "rd": [pltpu.VMEM((2 ** (k + 1), ny, nz, seg, 128), BF) for k in range(levels - 1)],
        "sum_b": comm_b.sum_scratch(),
    }
    for k in range(levels - 1):
        lists[f"sums{k}"] = comms[k + 1].sum_scratch()
    for name, items in lists.items():
        names += [f"{name}.{i}" for i in range(len(items))]
        shapes += items

    def body(*refs):
        flat = dict(zip(names, refs))
        r = {n: v for n, v in flat.items() if "." not in n}
        for name, items in lists.items():
            r[name] = [flat[f"{name}.{i}"] for i in range(len(items))]
        r["sums"] = [r[f"sums{k}"] for k in range(levels - 1)]
        cfg = dict(
            names=list(r), levels=levels, groups0=groups0, nx=nx, ny=ny, nz=nz, seg=seg,
            comms=comms, comm_b=comm_b, offsets=offsets,
        )
        main_kernel(cfg, *r.values())

    return pl.pallas_call(
        body,
        out_shape=(jax.ShapeDtypeStruct(rhs.shape, F32), jax.ShapeDtypeStruct(rhs.shape, F32)),
        in_specs=in_specs,
        out_specs=(vmem, vmem),
        scratch_shapes=shapes,
        compiler_params=pltpu.CompilerParams(
            collective_id=0, has_side_effects=True, vmem_limit_bytes=67043328
        ),
        cost_estimate=pl.CostEstimate(flops=10**10, bytes_accessed=3 * 10**7, transcendentals=0),
        name="refine_step",
    )(gathered, rhs, blocks, where, order, tri, placed, upper, updates)


def on_device(
    solution,
    right_side,
    block_values,
    block_columns,
    row_order,
    tri_inverses,
    lower_updates,
    upper_updates,
    update_rows,
):
    row_count = lax.axis_size("row")
    col_count = lax.axis_size("col")
    levels = row_count.bit_length() - 1
    per = solution.shape[0]
    seg = per // levels
    block_size = block_values.shape[2]
    per_block = per // block_size
    gathered = sent_to_all(solution.astype(BF), "row").reshape(row_count * per_block, block_size, -1)
    span0 = CORES * col_count * seg
    updates = update_rows.reshape(-1)
    placed = place_rows(lower_updates, updates, [span0 * 2**k for k in range(levels - 1)])
    ny = math.isqrt(col_count)
    correction, product = refine(
        levels,
        row_count // CORES,
        ny,
        col_count // ny,
        gathered,
        right_side,
        block_values.reshape(-1, block_size, block_size),
        block_columns,
        row_order,
        tri_inverses,
        placed,
        upper_updates,
        updates,
    )
    return solution + correction, right_side - product


def solution(mesh):
    in_specs = (
        P(("row", "col"), None),
        P(("row", "col"), None),
        P("row", "col", None, None),
        P("row", "col"),
        P(("row", "col")),
        P(("row", "col"), None),
        P(None, ("row", "col")),
        P(("row", "col"), None),
        P(),
    )
    out_specs = (P(("row", "col"), None), P(("row", "col"), None))
    return jax.shard_map(
        on_device, mesh=mesh, in_specs=in_specs, out_specs=out_specs, check_vma=False
    )
```

```python
import functools
import math

import jax
import jax.numpy as jnp
from jax import lax
from jax.experimental import pallas as pl
from jax.experimental.pallas import tpu as pltpu
from jax.sharding import PartitionSpec as P

MESH = pl.DeviceIdType.MESH
BF = jnp.bfloat16
F32 = jnp.float32
CORES = 2


def sent_to_all(x, axis):
    copies = jnp.broadcast_to(x, (lax.axis_size(axis), *x.shape))
    return lax.all_to_all(copies, axis, split_axis=0, concat_axis=0, tiled=True)


def dot(a, b):
    return jnp.dot(a, b, preferred_element_type=F32)


def place_kernel(spans, lower, updates, out, narrow, wide, placed, done, where, sem_in, sem_out, sem_idx):
    rows = 256
    step = 32
    row = lax.axis_index("row")
    copies = []
    start = 0
    for level, span in enumerate(spans):
        at = pl.ds(start, span)
        front = pl.multiple_of(level * (updates.shape[0] // len(spans)) + row // 2 ** (level + 1) * span, 1024)
        idx = pltpu.make_async_copy(updates.at[pl.ds(front, span)], where.at[at], sem_idx.at[level])
        idx.start()
        got = pltpu.make_async_copy(lower.at[at], narrow.at[at], sem_in.at[level])
        got.start()
        copies.append((idx, got))
        start += span

    start = 0
    puts = []
    for level, span in enumerate(spans):

        @pl.loop(0, 2 * span // rows)
        def _(i, start=start):
            at = pl.multiple_of(2 * start + i * rows, rows)
            placed[pl.ds(at, rows), :] = jnp.zeros((rows, placed.shape[1]), F32)

        for copy in copies[level]:
            copy.wait()

        @pl.loop(0, span // rows)
        def _(i, start=start):
            at = pl.ds(pl.multiple_of(start + i * rows, rows), rows)
            wide[at, :] = narrow[at, :].astype(F32)

        @pl.loop(0, span // step)
        def _(i, start=start):
            for j in range(step):
                u = start + i * step + j
                placed[2 * start + where[u]] = wide[u]

        block = out.shape[1]
        for part in range(2):
            first = (2 * start + part * span) // block

            @pl.loop(first, first + span // block)
            def _(i):
                done[i] = placed[pl.ds(pl.multiple_of(i * block, block), block), :].astype(BF)

            at = pl.ds(first, span // block)
            put = pltpu.make_async_copy(done.at[at], out.at[at], sem_out.at[level, part])
            put.start()
            puts.append(put)
        start += span
    for put in puts:
        put.wait()


def place_rows(lower, updates, spans):
    total, width = lower.shape
    blocks = 2 * total // 128
    hbm = pl.BlockSpec(memory_space=pl.ANY)
    return pl.pallas_call(
        functools.partial(place_kernel, spans),
        out_shape=jax.ShapeDtypeStruct((blocks, 128, width), BF),
        in_specs=[hbm, hbm],
        out_specs=hbm,
        scratch_shapes=[
            pltpu.VMEM((total, width), BF),
            pltpu.VMEM((total, width), F32),
            pltpu.VMEM((2 * total, width), F32),
            pltpu.VMEM((blocks, 128, width), BF),
            pltpu.SMEM((total,), jnp.int32),
            pltpu.SemaphoreType.DMA((len(spans),)),
            pltpu.SemaphoreType.DMA((len(spans), 2)),
            pltpu.SemaphoreType.DMA((len(spans),)),
        ],
        compiler_params=pltpu.CompilerParams(vmem_limit_bytes=56 * 2**20),
        cost_estimate=pl.CostEstimate(flops=10**10, bytes_accessed=10**7, transcendentals=0),
        name="place_rows",
    )(lower, updates)


class Comm:
    def __init__(self, sizes, rows):
        self.axes = [a for a in ("x", "y", "z") if sizes[a] > 1]
        self.n = {a: sizes[a] for a in self.axes}
        if len(self.axes) == 2:
            a, b = self.axes
            half = rows // 2
            self.parts = [((a, b), 0, half), ((b, a), half, half)]
        else:
            third = rows * 3 // 8
            self.parts = [
                (("y", "x", "z"), 0, third),
                (("z", "x", "y"), third, third),
                (("y", "z", "x"), 2 * third, rows - 2 * third),
            ]
        self.rows = rows
        steps = len(self.axes)
        self.messages = [(j, mask) for j in range(steps) for mask in range(2**j)]
        self.blocks = math.prod(self.n.values())

    def span(self, order, mask, at):
        index = {}
        for i, a in enumerate(order):
            index[a] = slice(1, self.n[a]) if mask >> i & 1 else at.get(a, 0)
        return index

    def sum_scratch(self):
        shapes = []
        for order, _, rows in self.parts:
            for j, mask in self.messages:
                dims = [self.n[a] - 1 for a in self.axes if mask >> order.index(a) & 1]
                shapes.append(pltpu.VMEM((self.n[order[j]] - 1, *dims, rows, 128), BF))
        return shapes


def main_kernel(cfg, *refs):
    names = cfg["names"]
    r = dict(zip(names, refs))
    levels, groups0, ny, nz, seg = cfg["levels"], cfg["groups0"], cfg["ny"], cfg["nz"], cfg["seg"]
    comms, comm_b = cfg["comms"], cfg["comm_b"]
    row = lax.axis_index("row")
    col = lax.axis_index("col")
    core = row % CORES
    other = 1 - core
    coord = {"x": row // CORES, "y": col // nz, "z": col % nz}
    size = {"x": cfg["nx"], "y": ny, "z": nz}
    plane = ny * nz * seg

    def device(axis, d, n):
        here = coord[axis]
        if axis == "x":
            base = here // n * n
            there = base + (here - base + d) % n
            return (there * CORES + core, col)
        there = (here + d) % n
        if axis == "y":
            return (row, there * nz + coord["z"])
        return (row, coord["y"] * nz + there)

    partner = (row + 1 - 2 * core, col)

    barrier = pltpu.get_barrier_semaphore()
    peers = [partner]
    for a in ("x", "y", "z"):
        peers += [device(a, d, size[a]) for d in range(1, size[a])]
    for peer in peers:
        pl.semaphore_signal(barrier, inc=1, device_id=peer, device_id_type=MESH)

    load = r["load_sem"]
    piece = r["blocks"].shape[0] // ny
    get_a = []
    for dy in [*range(1, ny), 0]:
        at = pl.ds((coord["y"] + dy) % ny * piece, piece)
        get_a.append(pltpu.make_async_copy(r["blocks"].at[at], r["al"].at[at], load.at[3 + levels + dy]))
        get_a[-1].start()
    get_p = pltpu.make_async_copy(r["tri"], r["tri_buf"], load.at[1])
    get_w = pltpu.make_async_copy(r["upper"], r["upper_buf"], load.at[2])

    per = r["rhs"].shape[0]

    def remote(src, dst, s, t, to):
        return pltpu.make_async_remote_copy(
            src_ref=src, dst_ref=dst, send_sem=s, recv_sem=t, device_id=to, device_id_type=MESH
        )

    def reduce(comm, ref, scratch, turn, ready):
        steps = len(comm.axes)
        count = len(comm.messages)
        slot = {m: i for i, m in enumerate(comm.messages)}
        recv = [scratch[p * count : (p + 1) * count] for p in range(len(comm.parts))]
        sends = r["send_sem"].at[turn]
        full = (1 << steps) - 1

        def copy(p, j, mask, d):
            order, r0, rows = comm.parts[p]
            a = order[j]
            index = comm.span(order, mask, {a: d})
            return remote(
                ref(index, pl.ds(r0, rows)),
                recv[p][slot[j, mask]].at[d - 1],
                sends,
                r["recv_sem"].at[turn, p, slot[j, mask]],
                device(a, d, comm.n[a]),
            )

        def send(p, j, mask):
            for d in range(1, comm.n[comm.parts[p][0][j]]):
                copy(p, j, mask, d).start()

        def send_last(p, d):
            for mask in sorted(range(2 ** (steps - 1)), key=lambda m: -bin(m).count("1")):
                copy(p, steps - 1, mask, d).start()

        arrived = set()

        def wait(p, j, mask):
            if (p, j, mask) not in arrived:
                arrived.add((p, j, mask))
                buf = recv[p][slot[j, mask]]
                sem = r["recv_sem"].at[turn, p, slot[j, mask]]
                remote(buf, buf, sends, sem, partner).wait_recv()

        def total(p, mask, low):
            order, r0, rows = comm.parts[p]
            froms = [recv[p][slot[j, mask]] for j in range(low, steps)]
            for j in range(low, steps):
                wait(p, j, mask)
            axes = [a for a in comm.axes if mask >> order.index(a) & 1]
            dims = [comm.n[a] - 1 for a in axes]

            def one(at):
                index = {a: 0 for a in order}
                for a, where in zip(axes, at):
                    index[a] = where + 1
                here = ref(index, pl.ds(r0, rows))
                value = here[...].astype(F32)
                for buf in froms:
                    for d in range(buf.shape[0]):
                        value = value + buf[(d, *at)].astype(F32)
                return here, value

            if not axes:
                return one(())[1]
            if len(dims) == 1:
                for i in range(dims[0]):
                    here, value = one((i,))
                    here[...] = value.astype(BF)
            else:

                @pl.loop(0, dims[0])
                def _(i):
                    for k in range(dims[1]):
                        here, value = one((i, k))
                        here[...] = value.astype(BF)

        parts = range(len(comm.parts))
        last = steps - 1
        ready(send_last)
        for i in reversed(range(last)):
            for mask in sorted(range(2**i), key=lambda m: -bin(m).count("1")):
                for p in parts:
                    total(p, mask | 1 << i, i + 1)
                    send(p, i, mask)
        out = [total(p, 0, 0) for p in parts]
        sent = sum((comm.blocks - 1) * rows for _, _, rows in comm.parts)
        everything = drain(sent)
        remote(everything, everything, sends, r["recv_sem"].at[turn, 0, 0], partner).wait_send()
        return [(r0, rows, out[p]) for p, (_, r0, rows) in enumerate(comm.parts)]

    def drain(rows):
        return r["al"].at[pl.ds(0, rows // 128)]

    def gather(level, value, buf, turn):
        comm = comms[level]
        steps = len(comm.axes)
        slot = {m: i for i, m in enumerate(comm.messages)}
        sends = r["send_sem"].at[turn]
        d2d_send = r["d2d_send"].at[turn, 0]
        d2d_recv = r["d2d_recv"].at[turn, 0]

        def block(index, side, rows):
            return buf.at[(index.get("x", 0), side, index["y"], index["z"], rows)]

        buf[0, 0, 0, 0] = value
        parts = range(len(comm.parts))

        def arrival(p, j, mask):
            return r["recv_sem"].at[turn, p, slot[j, mask]]

        def send(p, j, mask):
            order, r0, rows = comm.parts[p]
            a = order[j]
            n = comm.n[a]
            src = block(comm.span(order, mask, {}), 0, pl.ds(r0, rows))
            for d in range(1, n):
                dst = block(comm.span(order, mask, {a: n - d}), 0, pl.ds(r0, rows))
                remote(src, dst, sends, arrival(p, j, mask), device(a, d, n)).start()

        for j in range(steps):
            for p in parts:
                send(p, j, 0)
        remote(buf.at[0, 0, 0, 0], buf.at[0, 1, 0, 0], d2d_send, d2d_recv, partner).start()
        for j, mask in sorted(comm.messages, key=lambda m: (bin(m[1]).count("1"), m[0])):
            for p in parts:
                order, r0, rows = comm.parts[p]
                index = comm.span(order, mask | 1 << j, {})
                got = block(index, 0, pl.ds(r0, rows))
                remote(got, got, sends, arrival(p, j, mask), partner).wait_recv()
                if j + 1 < steps:
                    send(p, j + 1, mask | 1 << j)
                remote(got, block(index, 1, pl.ds(r0, rows)), d2d_send, d2d_recv, partner).start()
            for k in range(j + 2, steps):
                for p in parts:
                    send(p, k, mask | 1 << j)

        swap = remote(buf.at[:, 0], buf.at[:, 1], d2d_send, d2d_recv, partner)

        def close():
            swap.wait_send()
            sent = drain(sum((comm.blocks - 1) * rows for _, _, rows in comm.parts))
            remote(sent, sent, sends, arrival(0, 0, 0), partner).wait_send()

        return swap.wait_recv, close

    offsets = cfg["offsets"]
    natural = [
        ((yi + ny - coord["y"]) % ny, (zi + nz - coord["z"]) % nz) for yi in range(ny) for zi in range(nz)
    ]

    def place(nx, dx, ci, dy, dz):
        xi = (coord["x"] % nx + dx) % nx
        return ((xi * CORES + ci) * ny + (coord["y"] + dy) % ny) * nz + (coord["z"] + dz) % nz

    def triangle(level, buf, lower, joined):
        off = offsets[level]
        nx = buf.shape[0]
        here = coord["x"] % nx

        def panel(xi, ci):
            return r["tri_buf"][:, pl.ds(pl.multiple_of(off + (xi * CORES + ci) * plane, 128), plane)]

        def vector(xi, side):
            dx = (xi + nx - here) % nx
            return jnp.concatenate([buf[dx, side, dy, dz] for dy, dz in natural], 0)

        acc = dot(r["masked"][level, int(lower)], vector(here, 0))

        def mine(xi, acc):
            return acc + dot(panel(xi, core), vector(xi, 0))

        def theirs(xi, acc):
            return acc + dot(panel(xi, other), vector(xi, 1))

        if lower:
            acc = lax.fori_loop(0, here, mine, acc)
            joined()
            return lax.fori_loop(0, here + core, theirs, acc)
        acc = lax.fori_loop(here + 1, nx, mine, acc)
        joined()
        return lax.fori_loop(here + core, nx, theirs, acc)

    get_idx = []
    for k in range(levels - 1):
        m = cfg["offsets"][k + 1] - cfg["offsets"][k]
        first = pl.multiple_of(k * (r["updates"].shape[0] // (levels - 1)) + row // 2 ** (k + 1) * m, 1024)
        at = pl.ds(cfg["offsets"][k], m)
        get_idx.append(pltpu.make_async_copy(r["updates"].at[pl.ds(first, m)], r["targets"].at[at], load.at[3 + k]))
    al, sol, tb = r["al"], r["gathered"], r["tb"]
    kb = r["where"].shape[1]
    bpd = per // 128
    group = bpd * ny * nz

    def block_at(i, s):
        b = r["where"][i, s]
        return sol[b // group * bpd + b % bpd]

    def block_rows(dy):
        for dz in range(nz):
            to = (coord["y"] + dy) % ny * nz + (coord["z"] + dz) % nz
            for j in range(bpd):
                i = to * bpd + j
                left = jnp.concatenate([al[i * kb + s] for s in range(kb)], 1)
                right = jnp.concatenate([block_at(i, s) for s in range(kb)], 0)
                tb[dy, dz, j * 128 : (j + 1) * 128, :] = dot(left, right).astype(BF)

    def products(send):
        for n, dy in enumerate([*range(1, ny), 0]):
            get_a[n].wait()
            block_rows(dy)
            if n == 0:
                pl.semaphore_wait(barrier, len(peers))
            for p, (order, _, _) in enumerate(comm_b.parts):
                if order[-1] == "y" and dy > 0:
                    send(p, dy)
        for p, (order, _, _) in enumerate(comm_b.parts):
            if order[-1] == "z":
                for dz in range(1, nz):
                    send(p, dz)
        for copy in (get_l, get_p, get_w, *get_idx):
            copy.start()

        source = lax.broadcasted_iota(jnp.int32, (per, per), 0) + (row * ny * nz + col) * per
        to = jnp.broadcast_to(r["order"][...].reshape(1, per), (per, per))
        r["hot"][...] = jnp.where(source == to, 1.0, 0.0).T.astype(BF)
        get_p.wait()
        for level in range(levels):
            here = coord["x"] % 2**level * CORES + core
            own = r["tri_buf"][:, pl.ds(pl.multiple_of(offsets[level] + here * plane, 128), plane)].astype(F32)
            row_ids = col * seg + lax.broadcasted_iota(jnp.int32, (seg, plane), 0)
            col_ids = lax.broadcasted_iota(jnp.int32, (seg, plane), 1)
            r["masked"][level, 0] = jnp.where(col_ids >= row_ids, own, 0.0).astype(BF)
            r["masked"][level, 1] = jnp.where(col_ids < row_ids, own, 0.0).astype(BF)

    get_l = pltpu.make_async_copy(r["placed"], al, load.at[0])

    def first_b(index, rows):
        return tb.at[(index["y"], index["z"], rows)]

    for r0, rows, value in reduce(comm_b, first_b, r["sum_b"], 0, products):
        at = slice(r0, r0 + rows)
        r["product"][at, :] = value
        res = r["rhs"][at, :] - value
        hi = res.astype(BF)
        r["split"][at, 0:128] = hi
        r["split"][at, 128:256] = (res - hi.astype(F32)).astype(BF)
    both = dot(r["hot"][...], r["split"][...])
    r["vee"][...] = both[:, 0:128] + both[:, 128:256]

    turn = 1
    buf_a, buf_b = r["buf_a"], r["buf_b"]
    incoming = None
    for level in range(levels):
        e = r["vee"][level * seg : (level + 1) * seg, :]
        if level > 0:
            parts = incoming
            for r0, rows, value in parts:
                r["minus"][r0 : r0 + rows, :] = value
            e = e - r["minus"][...]
        cb = e.astype(BF)
        joined, close = gather(level, cb, buf_a[level], turn)
        turn += 1
        y = (triangle(level, buf_a[level], True, joined) + cb.astype(F32)).astype(BF)
        close()
        r["why"][level] = y
        if level == 0:
            get_l.wait()
        if level + 1 < levels:
            t, rd = r["t"][level], r["rd"][level]
            nx = t.shape[0]
            base = 2 * offsets[level] // 128
            half = ny // 2

            def update(dx, side, t=t, base=base, y=y, nx=nx):
                for h in range(2):
                    spots = [(dy, dz) for dy in range(h * half, (h + 1) * half) for dz in range(nz)]
                    rows = [al[base + place(nx, dx, (core + side) % CORES, dy, dz)] for dy, dz in spots]
                    res = dot(jnp.concatenate(rows, 0), y).astype(BF)
                    t[dx, side, h * half : (h + 1) * half] = res.reshape(half, nz, 128, 128)

            comm = comms[level + 1]

            def sums(send, t=t, rd=rd, nx=nx, comm=comm, turn=turn, update=update):
                swaps = []
                for xi in range(nx):
                    update(xi, 1)
                for p, (_, r0, rows) in enumerate(comm.parts):
                    at = pl.ds(r0, rows)
                    swap = remote(
                        t.at[:, 1, :, :, at],
                        rd.at[:, :, :, at],
                        r["d2d_send"].at[turn, p],
                        r["d2d_recv"].at[turn, p],
                        partner,
                    )
                    swap.start()
                    swaps.append(swap)
                for xi in range(nx):
                    update(xi, 0)
                for p, (order, r0, rows) in enumerate(comm.parts):
                    swaps[p].wait()

                    @pl.loop(0, nx * ny)
                    def _(i, at=slice(r0, r0 + rows)):
                        xi, yi = i // ny, i % ny
                        for zi in range(nz):
                            value = t[xi, 0, yi, zi, at].astype(F32) + rd[xi, yi, zi, at].astype(F32)
                            t[xi, 0, yi, zi, at] = value.astype(BF)

                    for d in range(1, comm.n[order[-1]]):
                        send(p, d)

            def first(index, rows, t=t):
                return t.at[(index["x"], 0, index["y"], index["z"], rows)]

            incoming = reduce(comm, first, r["sums"][level], turn, sums)
            turn += 1

    for copy in (get_w, *get_idx):
        copy.wait()
    xb = None
    for level in reversed(range(levels)):
        z = r["why"][level]
        if level + 1 < levels:
            src = buf_a[level + 1]
            wide, picked = r["wide"], r["picked"]
            xs = src.shape[0]

            for side in range(CORES):
                if side == 1:
                    joined()

                @pl.loop(0, xs * ny)
                def _(i, src=src, xs=xs, side=side):
                    dx, dy = i // ny, i % ny
                    for dz in range(nz):
                        to = pl.multiple_of(place(xs, dx, (core + side) % CORES, dy, dz) * 128, 128)
                        wide[pl.ds(to, 128), :] = src[dx, side, dy, dz].astype(F32)

            close_x()
            m = offsets[level + 1] - offsets[level]
            tile = picked.shape[0]
            tiles = m // tile // CORES
            where = r["targets"]
            step = 32
            rows = r["rows"]
            d2d_send, d2d_recv = r["d2d_send"].at[turn, 0], r["d2d_recv"].at[turn, 0]

            def product(i, acc, level=level):
                at = pl.ds(pl.multiple_of(offsets[level] + i * tile, 128), tile)
                return acc + dot(r["upper_buf"][:, at], rows[i])

            def chunk(i, acc, level=level, tiles=tiles):
                mine = core * tiles + i
                first = offsets[level] + mine * tile

                @pl.loop(0, tile // step)
                def _(u):
                    for v in range(step):
                        w = u * step + v
                        picked[w] = wide[where[first + w]]

                rows[mine] = picked[...].astype(BF)
                remote(rows.at[mine], rows.at[mine], d2d_send, d2d_recv, partner).start()
                return product(mine, acc)

            total = lax.fori_loop(0, tiles, chunk, jnp.zeros((seg, 128), F32))
            sent, got = rows.at[pl.ds(core * tiles, tiles)], rows.at[pl.ds(other * tiles, tiles)]
            remote(sent, got, d2d_send, d2d_recv, partner).wait()
            total = lax.fori_loop(other * tiles, (other + 1) * tiles, product, total)
            turn += 1
            z = (z.astype(F32) - total).astype(BF)
        joined, close = gather(level, z, buf_b[level], turn)
        turn += 1
        x = triangle(level, buf_b[level], False, joined)
        close()
        at = slice(level * seg, (level + 1) * seg)
        r["correction"][at, :] = x
        if level > 0:
            joined, close_x = gather(level, x.astype(BF), buf_a[level], turn)
            turn += 1


def refine(levels, nx, ny, nz, gathered, rhs, blocks, where, order, tri, placed, upper, updates):
    per = rhs.shape[0]
    seg = per // levels
    cols = ny * nz
    groups0 = CORES
    span0 = groups0 * cols * seg
    offsets = [span0 * (2**k - 1) for k in range(levels + 1)]
    comms = [Comm({"x": 2**k, "y": ny, "z": nz}, seg) for k in range(levels)]
    comm_b = Comm({"x": 1, "y": ny, "z": nz}, per)
    turns = 5 * levels - 2
    vmem = pl.BlockSpec(memory_space=pltpu.VMEM)
    smem = pl.BlockSpec(memory_space=pltpu.SMEM)
    hbm = pl.BlockSpec(memory_space=pl.ANY)
    ins = [
        ("gathered", vmem), ("rhs", vmem), ("blocks", hbm), ("where", smem), ("order", vmem),
        ("tri", hbm), ("placed", hbm), ("upper", hbm), ("updates", hbm),
    ]
    names = [n for n, _ in ins]
    in_specs = [s for _, s in ins]
    names += ["correction", "product"]
    front = lambda k: (2**k, CORES, ny, nz, seg, 128)
    scratch = {
        "al": pltpu.VMEM(blocks.shape, BF),
        "tri_buf": pltpu.VMEM(tri.shape, BF),
        "upper_buf": pltpu.VMEM(upper.shape, BF),
        "hot": pltpu.VMEM((per, per), BF),
        "tb": pltpu.VMEM((ny, nz, per, 128), BF),
        "split": pltpu.VMEM((per, 256), BF),
        "masked": pltpu.VMEM((levels, 2, seg, cols * seg), BF),
        "vee": pltpu.VMEM((per, 128), F32),
        "minus": pltpu.VMEM((seg, 128), F32),
        "why": pltpu.VMEM((levels, seg, 128), BF),
        "wide": pltpu.VMEM((2 ** (levels - 1) * span0, 128), F32),
        "picked": pltpu.VMEM((1024, 128), F32),
        "rows": pltpu.VMEM(((offsets[levels - 1] - offsets[levels - 2]) // 1024, 1024, 128), BF),
        "targets": pltpu.SMEM((offsets[levels - 1],), jnp.int32),
        "load_sem": pltpu.SemaphoreType.DMA((3 + levels + ny,)),
        "send_sem": pltpu.SemaphoreType.DMA((turns,)),
        "recv_sem": pltpu.SemaphoreType.DMA((turns, 3, 7)),
        "d2d_send": pltpu.SemaphoreType.DMA((turns, 3)),
        "d2d_recv": pltpu.SemaphoreType.DMA((turns, 3)),
    }
    names += list(scratch)
    shapes = list(scratch.values())
    lists = {
        "buf_a": [pltpu.VMEM(front(k), BF) for k in range(levels)],
        "buf_b": [pltpu.VMEM(front(k), BF) for k in range(levels)],
        "t": [pltpu.VMEM(front(k + 1), BF) for k in range(levels - 1)],
        "rd": [pltpu.VMEM((2 ** (k + 1), ny, nz, seg, 128), BF) for k in range(levels - 1)],
        "sum_b": comm_b.sum_scratch(),
    }
    for k in range(levels - 1):
        lists[f"sums{k}"] = comms[k + 1].sum_scratch()
    for name, items in lists.items():
        names += [f"{name}.{i}" for i in range(len(items))]
        shapes += items

    def body(*refs):
        flat = dict(zip(names, refs))
        r = {n: v for n, v in flat.items() if "." not in n}
        for name, items in lists.items():
            r[name] = [flat[f"{name}.{i}"] for i in range(len(items))]
        r["sums"] = [r[f"sums{k}"] for k in range(levels - 1)]
        cfg = dict(
            names=list(r), levels=levels, groups0=groups0, nx=nx, ny=ny, nz=nz, seg=seg,
            comms=comms, comm_b=comm_b, offsets=offsets,
        )
        main_kernel(cfg, *r.values())

    return pl.pallas_call(
        body,
        out_shape=(jax.ShapeDtypeStruct(rhs.shape, F32), jax.ShapeDtypeStruct(rhs.shape, F32)),
        in_specs=in_specs,
        out_specs=(vmem, vmem),
        scratch_shapes=shapes,
        compiler_params=pltpu.CompilerParams(
            collective_id=0, has_side_effects=True, vmem_limit_bytes=67043328
        ),
        cost_estimate=pl.CostEstimate(flops=10**10, bytes_accessed=3 * 10**7, transcendentals=0),
        name="refine_step",
    )(gathered, rhs, blocks, where, order, tri, placed, upper, updates)


def finish_kernel(old, rhs, correction, product, refined, residual):
    refined[...] = old[...] + correction[...]
    residual[...] = rhs[...] - product[...]


def finish(*arrays):
    vmem = pl.BlockSpec(memory_space=pltpu.VMEM)
    out = jax.ShapeDtypeStruct(arrays[0].shape, F32)
    return pl.pallas_call(
        finish_kernel, out_shape=(out, out), in_specs=[vmem] * 4, out_specs=(vmem, vmem), name="finish"
    )(*arrays)


def on_device(
    solution,
    right_side,
    block_values,
    block_columns,
    row_order,
    tri_inverses,
    lower_updates,
    upper_updates,
    update_rows,
):
    row_count = lax.axis_size("row")
    col_count = lax.axis_size("col")
    levels = row_count.bit_length() - 1
    per = solution.shape[0]
    seg = per // levels
    block_size = block_values.shape[2]
    per_block = per // block_size
    gathered = sent_to_all(solution.astype(BF), "row").reshape(row_count * per_block, block_size, -1)
    span0 = CORES * col_count * seg
    updates = update_rows.reshape(-1)
    placed = place_rows(lower_updates, updates, [span0 * 2**k for k in range(levels - 1)])
    ny = math.isqrt(col_count)
    correction, product = refine(
        levels,
        row_count // CORES,
        ny,
        col_count // ny,
        gathered,
        right_side,
        block_values.reshape(-1, block_size, block_size),
        block_columns,
        row_order,
        tri_inverses,
        placed,
        upper_updates,
        updates,
    )
    return finish(solution, right_side, correction, product)


def solution(mesh):
    in_specs = (
        P(("row", "col"), None),
        P(("row", "col"), None),
        P("row", "col", None, None),
        P("row", "col"),
        P(("row", "col")),
        P(("row", "col"), None),
        P(None, ("row", "col")),
        P(("row", "col"), None),
        P(),
    )
    out_specs = (P(("row", "col"), None), P(("row", "col"), None))
    return jax.shard_map(
        on_device, mesh=mesh, in_specs=in_specs, out_specs=out_specs, check_vma=False
    )
```

```python
import functools
import math

import jax
import jax.numpy as jnp
from jax import lax
from jax.experimental import pallas as pl
from jax.experimental.pallas import tpu as pltpu
from jax.sharding import PartitionSpec as P

MESH = pl.DeviceIdType.MESH
BF = jnp.bfloat16
F32 = jnp.float32
CORES = 2


def sent_to_all(x, axis):
    copies = jnp.broadcast_to(x, (lax.axis_size(axis), *x.shape))
    return lax.all_to_all(copies, axis, split_axis=0, concat_axis=0, tiled=True)


def dot(a, b):
    return jnp.dot(a, b, preferred_element_type=F32)


def place_kernel(spans, lower, updates, out, narrow, wide, placed, done, where, sem_in, sem_out, sem_idx):
    rows = 256
    step = 64
    pieces = sem_out.shape[1]
    row = lax.axis_index("row")
    copies = []
    start = 0
    for level, span in enumerate(spans):
        at = pl.ds(start, span)
        front = pl.multiple_of(level * (updates.shape[0] // len(spans)) + row // 2 ** (level + 1) * span, 1024)
        idx = pltpu.make_async_copy(updates.at[pl.ds(front, span)], where.at[at], sem_idx.at[level])
        idx.start()
        got = pltpu.make_async_copy(lower.at[at], narrow.at[at], sem_in.at[level])
        got.start()
        copies.append((idx, got))
        start += span

    start = 0
    puts = []
    for level, span in enumerate(spans):

        @pl.loop(0, 2 * span // rows)
        def _(i, start=start):
            at = pl.multiple_of(2 * start + i * rows, rows)
            placed[pl.ds(at, rows), :] = jnp.zeros((rows, placed.shape[1]), F32)

        for copy in copies[level]:
            copy.wait()

        @pl.loop(0, span // rows)
        def _(i, start=start):
            at = pl.ds(pl.multiple_of(start + i * rows, rows), rows)
            wide[at, :] = narrow[at, :].astype(F32)

        @pl.loop(0, span // step)
        def _(i, start=start):
            for j in range(step):
                u = start + i * step + j
                placed[2 * start + where[u]] = wide[u]

        block = out.shape[1]
        size = 2 * span // pieces // block
        for part in range(pieces):
            first = 2 * start // block + part * size

            @pl.loop(first, first + size)
            def _(i):
                done[i] = placed[pl.ds(pl.multiple_of(i * block, block), block), :].astype(BF)

            at = pl.ds(first, size)
            put = pltpu.make_async_copy(done.at[at], out.at[at], sem_out.at[level, part])
            put.start()
            puts.append(put)
        start += span
    for put in puts:
        put.wait()


def place_rows(lower, updates, spans):
    total, width = lower.shape
    blocks = 2 * total // 128
    hbm = pl.BlockSpec(memory_space=pl.ANY)
    return pl.pallas_call(
        functools.partial(place_kernel, spans),
        out_shape=jax.ShapeDtypeStruct((blocks, 128, width), BF),
        in_specs=[hbm, hbm],
        out_specs=hbm,
        scratch_shapes=[
            pltpu.VMEM((total, width), BF),
            pltpu.VMEM((total, width), F32),
            pltpu.VMEM((2 * total, width), F32),
            pltpu.VMEM((blocks, 128, width), BF),
            pltpu.SMEM((total,), jnp.int32),
            pltpu.SemaphoreType.DMA((len(spans),)),
            pltpu.SemaphoreType.DMA((len(spans), 4)),
            pltpu.SemaphoreType.DMA((len(spans),)),
        ],
        compiler_params=pltpu.CompilerParams(vmem_limit_bytes=56 * 2**20),
        cost_estimate=pl.CostEstimate(flops=10**10, bytes_accessed=10**7, transcendentals=0),
        name="place_rows",
    )(lower, updates)


class Comm:
    def __init__(self, sizes, rows):
        self.axes = [a for a in ("x", "y", "z") if sizes[a] > 1]
        self.n = {a: sizes[a] for a in self.axes}
        if len(self.axes) == 2:
            a, b = self.axes
            half = rows // 2
            self.parts = [((a, b), 0, half), ((b, a), half, half)]
        else:
            third = rows * 3 // 8
            self.parts = [
                (("y", "x", "z"), 0, third),
                (("z", "x", "y"), third, third),
                (("y", "z", "x"), 2 * third, rows - 2 * third),
            ]
        self.rows = rows
        steps = len(self.axes)
        self.messages = [(j, mask) for j in range(steps) for mask in range(2**j)]
        self.blocks = math.prod(self.n.values())

    def span(self, order, mask, at):
        index = {}
        for i, a in enumerate(order):
            index[a] = slice(1, self.n[a]) if mask >> i & 1 else at.get(a, 0)
        return index

    def sum_scratch(self):
        shapes = []
        for order, _, rows in self.parts:
            for j, mask in self.messages:
                dims = [self.n[a] - 1 for a in self.axes if mask >> order.index(a) & 1]
                shapes.append(pltpu.VMEM((self.n[order[j]] - 1, *dims, rows, 128), BF))
        return shapes


def main_kernel(cfg, *refs):
    names = cfg["names"]
    r = dict(zip(names, refs))
    levels, groups0, ny, nz, seg = cfg["levels"], cfg["groups0"], cfg["ny"], cfg["nz"], cfg["seg"]
    comms, comm_b = cfg["comms"], cfg["comm_b"]
    row = lax.axis_index("row")
    col = lax.axis_index("col")
    core = row % CORES
    other = 1 - core
    coord = {"x": row // CORES, "y": col // nz, "z": col % nz}
    size = {"x": cfg["nx"], "y": ny, "z": nz}
    plane = ny * nz * seg

    def device(axis, d, n):
        here = coord[axis]
        if axis == "x":
            base = here // n * n
            there = base + (here - base + d) % n
            return (there * CORES + core, col)
        there = (here + d) % n
        if axis == "y":
            return (row, there * nz + coord["z"])
        return (row, coord["y"] * nz + there)

    partner = (row + 1 - 2 * core, col)

    barrier = pltpu.get_barrier_semaphore()
    peers = [partner]
    for a in ("x", "y", "z"):
        peers += [device(a, d, size[a]) for d in range(1, size[a])]
    for peer in peers:
        pl.semaphore_signal(barrier, inc=1, device_id=peer, device_id_type=MESH)

    load = r["load_sem"]
    piece = r["blocks"].shape[0] // ny
    get_a = []
    for dy in [*range(1, ny), 0]:
        at = pl.ds((coord["y"] + dy) % ny * piece, piece)
        get_a.append(pltpu.make_async_copy(r["blocks"].at[at], r["al"].at[at], load.at[3 + levels + dy]))
        get_a[-1].start()
    get_p = pltpu.make_async_copy(r["tri"], r["tri_buf"], load.at[1])
    get_w = pltpu.make_async_copy(r["upper"], r["upper_buf"], load.at[2])

    per = r["rhs"].shape[0]

    def remote(src, dst, s, t, to):
        return pltpu.make_async_remote_copy(
            src_ref=src, dst_ref=dst, send_sem=s, recv_sem=t, device_id=to, device_id_type=MESH
        )

    def reduce(comm, ref, scratch, turn, ready):
        steps = len(comm.axes)
        count = len(comm.messages)
        slot = {m: i for i, m in enumerate(comm.messages)}
        recv = [scratch[p * count : (p + 1) * count] for p in range(len(comm.parts))]
        sends = r["send_sem"].at[turn]
        full = (1 << steps) - 1

        def copy(p, j, mask, d):
            order, r0, rows = comm.parts[p]
            a = order[j]
            index = comm.span(order, mask, {a: d})
            return remote(
                ref(index, pl.ds(r0, rows)),
                recv[p][slot[j, mask]].at[d - 1],
                sends,
                r["recv_sem"].at[turn, p, slot[j, mask]],
                device(a, d, comm.n[a]),
            )

        def send(p, j, mask):
            for d in range(1, comm.n[comm.parts[p][0][j]]):
                copy(p, j, mask, d).start()

        def send_last(p, d):
            for mask in sorted(range(2 ** (steps - 1)), key=lambda m: -bin(m).count("1")):
                copy(p, steps - 1, mask, d).start()

        arrived = set()

        def wait(p, j, mask):
            if (p, j, mask) not in arrived:
                arrived.add((p, j, mask))
                buf = recv[p][slot[j, mask]]
                sem = r["recv_sem"].at[turn, p, slot[j, mask]]
                remote(buf, buf, sends, sem, partner).wait_recv()

        def total(p, mask, low):
            order, r0, rows = comm.parts[p]
            froms = [recv[p][slot[j, mask]] for j in range(low, steps)]
            for j in range(low, steps):
                wait(p, j, mask)
            axes = [a for a in comm.axes if mask >> order.index(a) & 1]
            dims = [comm.n[a] - 1 for a in axes]

            def one(at):
                index = {a: 0 for a in order}
                for a, where in zip(axes, at):
                    index[a] = where + 1
                here = ref(index, pl.ds(r0, rows))
                value = here[...].astype(F32)
                for buf in froms:
                    for d in range(buf.shape[0]):
                        value = value + buf[(d, *at)].astype(F32)
                return here, value

            if not axes:
                return one(())[1]
            if len(dims) == 1:
                for i in range(dims[0]):
                    here, value = one((i,))
                    here[...] = value.astype(BF)
            else:

                @pl.loop(0, dims[0])
                def _(i):
                    for k in range(dims[1]):
                        here, value = one((i, k))
                        here[...] = value.astype(BF)

        parts = range(len(comm.parts))
        last = steps - 1
        ready(send_last)
        for i in reversed(range(last)):
            for mask in sorted(range(2**i), key=lambda m: -bin(m).count("1")):
                for p in parts:
                    total(p, mask | 1 << i, i + 1)
                    send(p, i, mask)
        out = [total(p, 0, 0) for p in parts]
        sent = sum((comm.blocks - 1) * rows for _, _, rows in comm.parts)
        everything = drain(sent)
        remote(everything, everything, sends, r["recv_sem"].at[turn, 0, 0], partner).wait_send()
        return [(r0, rows, out[p]) for p, (_, r0, rows) in enumerate(comm.parts)]

    def drain(rows):
        return r["al"].at[pl.ds(0, rows // 128)]

    def gather(level, value, buf, turn):
        comm = comms[level]
        steps = len(comm.axes)
        slot = {m: i for i, m in enumerate(comm.messages)}
        sends = r["send_sem"].at[turn]
        d2d_send = r["d2d_send"].at[turn, 0]
        d2d_recv = r["d2d_recv"].at[turn, 0]

        def block(index, side, rows):
            return buf.at[(index.get("x", 0), side, index["y"], index["z"], rows)]

        buf[0, 0, 0, 0] = value
        parts = range(len(comm.parts))

        def arrival(p, j, mask):
            return r["recv_sem"].at[turn, p, slot[j, mask]]

        def send(p, j, mask):
            order, r0, rows = comm.parts[p]
            a = order[j]
            n = comm.n[a]
            src = block(comm.span(order, mask, {}), 0, pl.ds(r0, rows))
            for d in range(1, n):
                dst = block(comm.span(order, mask, {a: n - d}), 0, pl.ds(r0, rows))
                remote(src, dst, sends, arrival(p, j, mask), device(a, d, n)).start()

        for j in range(steps):
            for p in parts:
                send(p, j, 0)
        remote(buf.at[0, 0, 0, 0], buf.at[0, 1, 0, 0], d2d_send, d2d_recv, partner).start()
        for j, mask in sorted(comm.messages, key=lambda m: (bin(m[1]).count("1"), m[0])):
            for p in parts:
                order, r0, rows = comm.parts[p]
                index = comm.span(order, mask | 1 << j, {})
                got = block(index, 0, pl.ds(r0, rows))
                remote(got, got, sends, arrival(p, j, mask), partner).wait_recv()
                if j + 1 < steps:
                    send(p, j + 1, mask | 1 << j)
                remote(got, block(index, 1, pl.ds(r0, rows)), d2d_send, d2d_recv, partner).start()
            for k in range(j + 2, steps):
                for p in parts:
                    send(p, k, mask | 1 << j)

        swap = remote(buf.at[:, 0], buf.at[:, 1], d2d_send, d2d_recv, partner)

        def close():
            swap.wait_send()
            sent = drain(sum((comm.blocks - 1) * rows for _, _, rows in comm.parts))
            remote(sent, sent, sends, arrival(0, 0, 0), partner).wait_send()

        return swap.wait_recv, close

    offsets = cfg["offsets"]
    natural = [
        ((yi + ny - coord["y"]) % ny, (zi + nz - coord["z"]) % nz) for yi in range(ny) for zi in range(nz)
    ]

    def place(nx, dx, ci, dy, dz):
        xi = (coord["x"] % nx + dx) % nx
        return ((xi * CORES + ci) * ny + (coord["y"] + dy) % ny) * nz + (coord["z"] + dz) % nz

    def triangle(level, buf, lower, joined):
        off = offsets[level]
        nx = buf.shape[0]
        here = coord["x"] % nx

        def panel(xi, ci):
            return r["tri_buf"][:, pl.ds(pl.multiple_of(off + (xi * CORES + ci) * plane, 128), plane)]

        def vector(xi, side):
            dx = (xi + nx - here) % nx
            return jnp.concatenate([buf[dx, side, dy, dz] for dy, dz in natural], 0)

        acc = dot(r["masked"][level, int(lower)], vector(here, 0))

        def mine(xi, acc):
            return acc + dot(panel(xi, core), vector(xi, 0))

        def theirs(xi, acc):
            return acc + dot(panel(xi, other), vector(xi, 1))

        if lower:
            acc = lax.fori_loop(0, here, mine, acc)
            joined()
            return lax.fori_loop(0, here + core, theirs, acc)
        acc = lax.fori_loop(here + 1, nx, mine, acc)
        joined()
        return lax.fori_loop(here + core, nx, theirs, acc)

    get_idx = []
    for k in range(levels - 1):
        m = cfg["offsets"][k + 1] - cfg["offsets"][k]
        first = pl.multiple_of(k * (r["updates"].shape[0] // (levels - 1)) + row // 2 ** (k + 1) * m, 1024)
        at = pl.ds(cfg["offsets"][k], m)
        get_idx.append(pltpu.make_async_copy(r["updates"].at[pl.ds(first, m)], r["targets"].at[at], load.at[3 + k]))
    al, sol, tb = r["al"], r["gathered"], r["tb"]
    kb = r["where"].shape[1]
    bpd = per // 128
    group = bpd * ny * nz

    def block_at(i, s):
        b = r["where"][i, s]
        return sol[b // group * bpd + b % bpd]

    def block_rows(dy):
        for dz in range(nz):
            to = (coord["y"] + dy) % ny * nz + (coord["z"] + dz) % nz
            for j in range(bpd):
                i = to * bpd + j
                left = jnp.concatenate([al[i * kb + s] for s in range(kb)], 1)
                right = jnp.concatenate([block_at(i, s) for s in range(kb)], 0)
                tb[dy, dz, j * 128 : (j + 1) * 128, :] = dot(left, right).astype(BF)

    def products(send):
        for n, dy in enumerate([*range(1, ny), 0]):
            get_a[n].wait()
            block_rows(dy)
            if n == 0:
                pl.semaphore_wait(barrier, len(peers))
            for p, (order, _, _) in enumerate(comm_b.parts):
                if order[-1] == "y" and dy > 0:
                    send(p, dy)
        for p, (order, _, _) in enumerate(comm_b.parts):
            if order[-1] == "z":
                for dz in range(1, nz):
                    send(p, dz)
        for copy in (get_l, get_p, get_w, *get_idx):
            copy.start()

        source = lax.broadcasted_iota(jnp.int32, (per, per), 0) + (row * ny * nz + col) * per
        to = jnp.broadcast_to(r["order"][...].reshape(1, per), (per, per))
        r["hot"][...] = jnp.where(source == to, 1.0, 0.0).T.astype(BF)
        get_p.wait()
        for level in range(levels):
            here = coord["x"] % 2**level * CORES + core
            own = r["tri_buf"][:, pl.ds(pl.multiple_of(offsets[level] + here * plane, 128), plane)].astype(F32)
            row_ids = col * seg + lax.broadcasted_iota(jnp.int32, (seg, plane), 0)
            col_ids = lax.broadcasted_iota(jnp.int32, (seg, plane), 1)
            r["masked"][level, 0] = jnp.where(col_ids >= row_ids, own, 0.0).astype(BF)
            r["masked"][level, 1] = jnp.where(col_ids < row_ids, own, 0.0).astype(BF)

    get_l = pltpu.make_async_copy(r["placed"], al, load.at[0])

    def first_b(index, rows):
        return tb.at[(index["y"], index["z"], rows)]

    for r0, rows, value in reduce(comm_b, first_b, r["sum_b"], 0, products):
        at = slice(r0, r0 + rows)
        r["product"][at, :] = value
        res = r["rhs"][at, :] - value
        hi = res.astype(BF)
        r["split"][at, 0:128] = hi
        r["split"][at, 128:256] = (res - hi.astype(F32)).astype(BF)
    both = dot(r["hot"][...], r["split"][...])
    r["vee"][...] = both[:, 0:128] + both[:, 128:256]

    turn = 1
    buf_a, buf_b = r["buf_a"], r["buf_b"]
    incoming = None
    for level in range(levels):
        e = r["vee"][level * seg : (level + 1) * seg, :]
        if level > 0:
            parts = incoming
            for r0, rows, value in parts:
                r["minus"][r0 : r0 + rows, :] = value
            e = e - r["minus"][...]
        cb = e.astype(BF)
        joined, close = gather(level, cb, buf_a[level], turn)
        turn += 1
        y = (triangle(level, buf_a[level], True, joined) + cb.astype(F32)).astype(BF)
        close()
        r["why"][level] = y
        if level == 0:
            get_l.wait()
        if level + 1 < levels:
            t, rd = r["t"][level], r["rd"][level]
            nx = t.shape[0]
            base = 2 * offsets[level] // 128
            half = ny // 2

            def update(dx, side, t=t, base=base, y=y, nx=nx):
                for h in range(2):
                    spots = [(dy, dz) for dy in range(h * half, (h + 1) * half) for dz in range(nz)]
                    rows = [al[base + place(nx, dx, (core + side) % CORES, dy, dz)] for dy, dz in spots]
                    res = dot(jnp.concatenate(rows, 0), y).astype(BF)
                    t[dx, side, h * half : (h + 1) * half] = res.reshape(half, nz, 128, 128)

            comm = comms[level + 1]

            def sums(send, t=t, rd=rd, nx=nx, comm=comm, turn=turn, update=update):
                swaps = []
                for xi in range(nx):
                    update(xi, 1)
                for p, (_, r0, rows) in enumerate(comm.parts):
                    at = pl.ds(r0, rows)
                    swap = remote(
                        t.at[:, 1, :, :, at],
                        rd.at[:, :, :, at],
                        r["d2d_send"].at[turn, p],
                        r["d2d_recv"].at[turn, p],
                        partner,
                    )
                    swap.start()
                    swaps.append(swap)
                for xi in range(nx):
                    update(xi, 0)
                for p, (order, r0, rows) in enumerate(comm.parts):
                    swaps[p].wait()

                    @pl.loop(0, nx * ny)
                    def _(i, at=slice(r0, r0 + rows)):
                        xi, yi = i // ny, i % ny
                        for zi in range(nz):
                            value = t[xi, 0, yi, zi, at].astype(F32) + rd[xi, yi, zi, at].astype(F32)
                            t[xi, 0, yi, zi, at] = value.astype(BF)

                    for d in range(1, comm.n[order[-1]]):
                        send(p, d)

            def first(index, rows, t=t):
                return t.at[(index["x"], 0, index["y"], index["z"], rows)]

            incoming = reduce(comm, first, r["sums"][level], turn, sums)
            turn += 1

    for copy in (get_w, *get_idx):
        copy.wait()
    xb = None
    for level in reversed(range(levels)):
        z = r["why"][level]
        if level + 1 < levels:
            src = buf_a[level + 1]
            wide, picked = r["wide"], r["picked"]
            xs = src.shape[0]

            for side in range(CORES):
                if side == 1:
                    joined()

                @pl.loop(0, xs * ny)
                def _(i, src=src, xs=xs, side=side):
                    dx, dy = i // ny, i % ny
                    for dz in range(nz):
                        to = pl.multiple_of(place(xs, dx, (core + side) % CORES, dy, dz) * 128, 128)
                        wide[pl.ds(to, 128), :] = src[dx, side, dy, dz].astype(F32)

            close_x()
            m = offsets[level + 1] - offsets[level]
            tile = picked.shape[0]
            tiles = m // tile // CORES
            where = r["targets"]
            step = 64
            rows = r["rows"]
            d2d_send, d2d_recv = r["d2d_send"].at[turn, 0], r["d2d_recv"].at[turn, 0]

            def product(i, acc, level=level):
                at = pl.ds(pl.multiple_of(offsets[level] + i * tile, 128), tile)
                return acc + dot(r["upper_buf"][:, at], rows[i])

            def chunk(i, acc, level=level, tiles=tiles):
                mine = core * tiles + i
                first = offsets[level] + mine * tile

                @pl.loop(0, tile // step)
                def _(u):
                    for v in range(step):
                        w = u * step + v
                        picked[w] = wide[where[first + w]]

                rows[mine] = picked[...].astype(BF)
                remote(rows.at[mine], rows.at[mine], d2d_send, d2d_recv, partner).start()
                return product(mine, acc)

            total = lax.fori_loop(0, tiles, chunk, jnp.zeros((seg, 128), F32))
            sent, got = rows.at[pl.ds(core * tiles, tiles)], rows.at[pl.ds(other * tiles, tiles)]
            remote(sent, got, d2d_send, d2d_recv, partner).wait()
            total = lax.fori_loop(other * tiles, (other + 1) * tiles, product, total)
            turn += 1
            z = (z.astype(F32) - total).astype(BF)
        joined, close = gather(level, z, buf_b[level], turn)
        turn += 1
        x = triangle(level, buf_b[level], False, joined)
        close()
        at = slice(level * seg, (level + 1) * seg)
        r["correction"][at, :] = x
        if level > 0:
            joined, close_x = gather(level, x.astype(BF), buf_a[level], turn)
            turn += 1


def refine(levels, nx, ny, nz, gathered, rhs, blocks, where, order, tri, placed, upper, updates):
    per = rhs.shape[0]
    seg = per // levels
    cols = ny * nz
    groups0 = CORES
    span0 = groups0 * cols * seg
    offsets = [span0 * (2**k - 1) for k in range(levels + 1)]
    comms = [Comm({"x": 2**k, "y": ny, "z": nz}, seg) for k in range(levels)]
    comm_b = Comm({"x": 1, "y": ny, "z": nz}, per)
    turns = 5 * levels - 2
    vmem = pl.BlockSpec(memory_space=pltpu.VMEM)
    smem = pl.BlockSpec(memory_space=pltpu.SMEM)
    hbm = pl.BlockSpec(memory_space=pl.ANY)
    ins = [
        ("gathered", vmem), ("rhs", vmem), ("blocks", hbm), ("where", smem), ("order", vmem),
        ("tri", hbm), ("placed", hbm), ("upper", hbm), ("updates", hbm),
    ]
    names = [n for n, _ in ins]
    in_specs = [s for _, s in ins]
    names += ["correction", "product"]
    front = lambda k: (2**k, CORES, ny, nz, seg, 128)
    scratch = {
        "al": pltpu.VMEM(blocks.shape, BF),
        "tri_buf": pltpu.VMEM(tri.shape, BF),
        "upper_buf": pltpu.VMEM(upper.shape, BF),
        "hot": pltpu.VMEM((per, per), BF),
        "tb": pltpu.VMEM((ny, nz, per, 128), BF),
        "split": pltpu.VMEM((per, 256), BF),
        "masked": pltpu.VMEM((levels, 2, seg, cols * seg), BF),
        "vee": pltpu.VMEM((per, 128), F32),
        "minus": pltpu.VMEM((seg, 128), F32),
        "why": pltpu.VMEM((levels, seg, 128), BF),
        "wide": pltpu.VMEM((2 ** (levels - 1) * span0, 128), F32),
        "picked": pltpu.VMEM((1024, 128), F32),
        "rows": pltpu.VMEM(((offsets[levels - 1] - offsets[levels - 2]) // 1024, 1024, 128), BF),
        "targets": pltpu.SMEM((offsets[levels - 1],), jnp.int32),
        "load_sem": pltpu.SemaphoreType.DMA((3 + levels + ny,)),
        "send_sem": pltpu.SemaphoreType.DMA((turns,)),
        "recv_sem": pltpu.SemaphoreType.DMA((turns, 3, 7)),
        "d2d_send": pltpu.SemaphoreType.DMA((turns, 3)),
        "d2d_recv": pltpu.SemaphoreType.DMA((turns, 3)),
    }
    names += list(scratch)
    shapes = list(scratch.values())
    lists = {
        "buf_a": [pltpu.VMEM(front(k), BF) for k in range(levels)],
        "buf_b": [pltpu.VMEM(front(k), BF) for k in range(levels)],
        "t": [pltpu.VMEM(front(k + 1), BF) for k in range(levels - 1)],
        "rd": [pltpu.VMEM((2 ** (k + 1), ny, nz, seg, 128), BF) for k in range(levels - 1)],
        "sum_b": comm_b.sum_scratch(),
    }
    for k in range(levels - 1):
        lists[f"sums{k}"] = comms[k + 1].sum_scratch()
    for name, items in lists.items():
        names += [f"{name}.{i}" for i in range(len(items))]
        shapes += items

    def body(*refs):
        flat = dict(zip(names, refs))
        r = {n: v for n, v in flat.items() if "." not in n}
        for name, items in lists.items():
            r[name] = [flat[f"{name}.{i}"] for i in range(len(items))]
        r["sums"] = [r[f"sums{k}"] for k in range(levels - 1)]
        cfg = dict(
            names=list(r), levels=levels, groups0=groups0, nx=nx, ny=ny, nz=nz, seg=seg,
            comms=comms, comm_b=comm_b, offsets=offsets,
        )
        main_kernel(cfg, *r.values())

    return pl.pallas_call(
        body,
        out_shape=(jax.ShapeDtypeStruct(rhs.shape, F32), jax.ShapeDtypeStruct(rhs.shape, F32)),
        in_specs=in_specs,
        out_specs=(vmem, vmem),
        scratch_shapes=shapes,
        compiler_params=pltpu.CompilerParams(
            collective_id=0, has_side_effects=True, vmem_limit_bytes=67043328
        ),
        cost_estimate=pl.CostEstimate(flops=10**10, bytes_accessed=3 * 10**7, transcendentals=0),
        name="refine_step",
    )(gathered, rhs, blocks, where, order, tri, placed, upper, updates)


def finish_kernel(old, rhs, correction, product, refined, residual):
    refined[...] = old[...] + correction[...]
    residual[...] = rhs[...] - product[...]


def finish(*arrays):
    vmem = pl.BlockSpec(memory_space=pltpu.VMEM)
    out = jax.ShapeDtypeStruct(arrays[0].shape, F32)
    return pl.pallas_call(
        finish_kernel, out_shape=(out, out), in_specs=[vmem] * 4, out_specs=(vmem, vmem), name="finish"
    )(*arrays)


def on_device(
    solution,
    right_side,
    block_values,
    block_columns,
    row_order,
    tri_inverses,
    lower_updates,
    upper_updates,
    update_rows,
):
    row_count = lax.axis_size("row")
    col_count = lax.axis_size("col")
    levels = row_count.bit_length() - 1
    per = solution.shape[0]
    seg = per // levels
    block_size = block_values.shape[2]
    per_block = per // block_size
    gathered = sent_to_all(solution.astype(BF), "row").reshape(row_count * per_block, block_size, -1)
    span0 = CORES * col_count * seg
    updates = update_rows.reshape(-1)
    placed = place_rows(lower_updates, updates, [span0 * 2**k for k in range(levels - 1)])
    ny = math.isqrt(col_count)
    correction, product = refine(
        levels,
        row_count // CORES,
        ny,
        col_count // ny,
        gathered,
        right_side,
        block_values.reshape(-1, block_size, block_size),
        block_columns,
        row_order,
        tri_inverses,
        placed,
        upper_updates,
        updates,
    )
    return finish(solution, right_side, correction, product)


def solution(mesh):
    in_specs = (
        P(("row", "col"), None),
        P(("row", "col"), None),
        P("row", "col", None, None),
        P("row", "col"),
        P(("row", "col")),
        P(("row", "col"), None),
        P(None, ("row", "col")),
        P(("row", "col"), None),
        P(),
    )
    out_specs = (P(("row", "col"), None), P(("row", "col"), None))
    return jax.shard_map(
        on_device, mesh=mesh, in_specs=in_specs, out_specs=out_specs, check_vma=False
    )
```
